16 devices in a mesh: rep: 1, dp: 16 (over x, y, z, core).
Axes of the slice: x: 2, y: 2, z: 2, core: 2. Of those that a mesh axis runs over, the one named last changes fastest.
Arguments:
- g_w_gate: bfloat16 [16, 2, 896, 2560], P(('rep', 'dp'))
- g_w_up: bfloat16 [16, 2, 896, 2560], P(('rep', 'dp'))
- g_w_down: bfloat16 [16, 2, 2560, 896], P(('rep', 'dp'))
- w_gate: bfloat16 [2, 896, 2560], replicated
- w_up: bfloat16 [2, 896, 2560], replicated
- w_down: bfloat16 [2, 2560, 896], replicated
- m_w_gate: float32 [2, 896, 2560], P(None, 'dp')
- m_w_up: float32 [2, 896, 2560], P(None, 'dp')
- m_w_down: float32 [2, 2560, 896], P(None, 'dp')
- v_w_gate: float32 [2, 896, 2560], P(None, 'dp')
- v_w_up: float32 [2, 896, 2560], P(None, 'dp')
- v_w_down: float32 [2, 2560, 896], P(None, 'dp')
Outputs:
- output 1: bfloat16 [2, 896, 2560], P('rep')
- output 2: bfloat16 [2, 896, 2560], P('rep')
- output 3: bfloat16 [2, 2560, 896], P('rep')
- output 4: float32 [2, 896, 2560], P('rep', 'dp')
- output 5: float32 [2, 896, 2560], P('rep', 'dp')
- output 6: float32 [2, 2560, 896], P('rep', 'dp')
- output 7: float32 [2, 896, 2560], P('rep', 'dp')
- output 8: float32 [2, 896, 2560], P('rep', 'dp')
- output 9: float32 [2, 2560, 896], P('rep', 'dp')
All inputs are finite; a program needn't handle non-finite values.
Results may differ from the reference program's by a relative error of at most 0.022.
Values are sent between devices in bfloat16 or wider.
A program may use at most 2 GiB of HBM per device.

```python
import jax
import jax.numpy as jnp
from jax import lax

DEVICES = 16
D = 896
FF = 2560
LAYERS = 2
NAMES = ("w_gate", "w_up", "w_down")
SHAPES = {"w_gate": (LAYERS, D, FF), "w_up": (LAYERS, D, FF), "w_down": (LAYERS, FF, D)}


def setup_inputs(seed: int = 0, part: int = 0) -> dict:
    kz, *keys = jax.random.split(jax.random.key(seed), 1 + 5 * len(NAMES))
    loud = 2.0 ** jax.random.uniform(kz, (), jnp.float32, -1.0, 1.0)
    drawn = {}
    for name, key, both in zip(NAMES, keys[:3], keys[3:6], strict=True):
        own = jax.random.normal(jax.random.fold_in(key, part), (DEVICES, *SHAPES[name]), jnp.float32)
        shared = jax.random.normal(jax.random.fold_in(both, part), SHAPES[name], jnp.float32)
        drawn["g_" + name] = (loud * (0.7 * shared / DEVICES + 0.7 * own * DEVICES**-0.5)).astype(jnp.bfloat16)
    for name, key in zip(NAMES, keys[6:9], strict=True):
        drawn[name] = (jax.random.normal(key, SHAPES[name], jnp.float32) * SHAPES[name][1] ** -0.5).astype(jnp.bfloat16)
    for name, key in zip(NAMES, keys[9:12], strict=True):
        drawn["m_" + name] = loud * 0.5 * jax.random.normal(key, SHAPES[name], jnp.float32)
    for name, key in zip(NAMES, keys[12:15], strict=True):
        drawn["v_" + name] = loud * loud * jax.random.uniform(key, SHAPES[name], jnp.float32, 0.5, 1.5)
    return drawn


def adamw(w, m, v, g):
    m = 0.9 * m + 0.1 * g
    v = 0.95 * v + 0.05 * g * g
    step = m * lax.rsqrt(v + 1e-8) + 0.1 * w
    return (w - 0.02 * step).astype(jnp.bfloat16), m, v


def reference(g_w_gate, g_w_up, g_w_down, w_gate, w_up, w_down, m_w_gate, m_w_up, m_w_down, v_w_gate, v_w_up, v_w_down):
    def total(terms):
        return lax.scan(lambda so_far, term: (so_far + term.astype(jnp.float32), None), jnp.zeros(terms.shape[1:], jnp.float32), terms)[0]

    gradients = [total(terms).astype(jnp.bfloat16).astype(jnp.float32) for terms in (g_w_gate, g_w_up, g_w_down)]
    new = [
        adamw(w.astype(jnp.float32), m, v, g)
        for w, m, v, g in zip((w_gate, w_up, w_down), (m_w_gate, m_w_up, m_w_down), (v_w_gate, v_w_up, v_w_down), gradients, strict=True)
    ]
    return tuple(one[which] for which in range(3) for one in new)
```

```python
import functools

import jax
import jax.numpy as jnp
from jax import lax
from jax.experimental import pallas as pl
from jax.experimental.pallas import tpu as pltpu
from jax.sharding import PartitionSpec as P

MESH = pl.DeviceIdType.MESH
F32, BF16 = jnp.float32, jnp.bfloat16
N = 16
LAYERS = 2
TILES = 70
AXES = ((8, 4, 2), (4, 2, 8), (2, 8, 4))
SUB = 10
T = TILES // SUB
CHUNKS = LAYERS * SUB
LEAD = 2
RING0 = 2 * LEAD + 2
RING = 4
VM = pltpu.VMEM
ST1, ST2, ST3, AG3, AG2, AG1, ST0, AG0 = range(8)


def add_into(dst, *srcs):
    total = srcs[0][...].astype(F32)
    for one in srcs[1:]:
        total = total + one[...].astype(F32)
    dst[...] = total.astype(BF16)


def kernel(*refs):
    g, w, m, v = (refs[i : i + 3] for i in range(0, 12, 3))
    moments, new_w = refs[12:14]
    wo = [new_w.at[k] for k in range(3)]
    mo, vo = ([moments.at[i, k] for k in range(3)] for i in range(2))
    D, R1, R2, R3, O1, O2, O3, O4, W, s0r, rr, a0r, snd, ld, mv = refs[14:]
    me = lax.axis_index("dp")

    def bit(b):
        return lax.rem(me // b, 2)

    def flip(i, b):
        return i + b - 2 * b * bit(b)

    core = bit(1)
    mate = flip(me, 1)

    def remote(src, dst, send, recv, to):
        return pltpu.make_async_remote_copy(src, dst, send, recv, device_id={"dp": to}, device_id_type=MESH)

    def arrived(ref, sem):
        remote(ref, ref, snd.at[ST0, 0], sem, mate).wait_recv()

    def loaded(ref, sem):
        pltpu.make_async_copy(ref, ref, sem).wait()

    def where(ch):
        return ch // SUB, pl.ds(lax.rem(ch, SUB) * T, T)

    def owner(k, e1, e2, e3, c):
        b1, b2, b3 = AXES[k]
        return e1 * b1 + e2 * b2 + e3 * b3 + c

    def send_raw(ch):
        l, rows = where(ch)
        for k in range(3):
            for p in range(8):
                j = owner(k, p // 4, p // 2 % 2, p % 2, 1 - core)
                remote(g[k].at[l, j, rows], D.at[k, ch, p], snd.at[ST0, k], s0r.at[k, lax.rem(ch, RING0)], mate).start()

    def load_own(which, ch):
        l, rows = where(ch)
        slot = lax.rem(ch, 2)
        for k in range(3):
            b1, b2, b3 = AXES[k]
            m1, m2, m3 = bit(b1), bit(b2), bit(b3)
            if which == 0:
                for q in range(4):
                    j = owner(k, 1 - m1, q // 2, q % 2, core)
                    pltpu.make_async_copy(g[k].at[l, j, rows], O1.at[k, slot, q], ld.at[0, k, slot]).start()
            elif which == 1:
                for q in range(2):
                    j = owner(k, m1, 1 - m2, q, core)
                    pltpu.make_async_copy(g[k].at[l, j, rows], O2.at[k, slot, q], ld.at[1, k, slot]).start()
            elif which == 2:
                j = owner(k, m1, m2, 1 - m3, core)
                pltpu.make_async_copy(g[k].at[l, j, rows], O3.at[k, slot], ld.at[2, k, slot]).start()
            else:
                pltpu.make_async_copy(g[k].at[l, me, rows], O4.at[k, slot], ld.at[3, k, slot]).start()
                pltpu.make_async_copy(w[k].at[l, me, rows], W.at[k, slot], ld.at[4, k, slot]).start()

    def stage1(ch):
        slot = lax.rem(ch, 2)
        for k in range(3):
            b1, b2, b3 = AXES[k]
            base = 4 * (1 - bit(b1))
            arrived(D.at[k, ch], s0r.at[k, lax.rem(ch, RING0)])
            loaded(O1.at[k, slot], ld.at[0, k, slot])

            def one(q, _):
                add_into(D.at[k, ch, base + q], O1.at[k, slot, q], D.at[k, ch, base + q])
                return 0

            lax.fori_loop(0, 4, one, 0)
            remote(D.at[k, ch, pl.ds(base, 4)], R1.at[k, ch], snd.at[ST1, k], rr.at[ST1, k, lax.rem(ch, RING)], flip(me, b1)).start()

    def stage2(ch):
        slot, ring = lax.rem(ch, 2), lax.rem(ch, RING)
        for k in range(3):
            b1, b2, b3 = AXES[k]
            half = 2 * (1 - bit(b2))
            base = 4 * bit(b1) + half
            arrived(R1.at[k, ch], rr.at[ST1, k, ring])
            loaded(O2.at[k, slot], ld.at[1, k, slot])

            def one(q, _):
                add_into(D.at[k, ch, base + q], O2.at[k, slot, q], D.at[k, ch, base + q], R1.at[k, ch, half + q])
                return 0

            lax.fori_loop(0, 2, one, 0)
            remote(D.at[k, ch, pl.ds(base, 2)], R2.at[k, ch], snd.at[ST2, k], rr.at[ST2, k, ring], flip(me, b2)).start()

    def stage3(ch):
        slot, ring = lax.rem(ch, 2), lax.rem(ch, RING)
        for k in range(3):
            b1, b2, b3 = AXES[k]
            m1, m2, n3 = bit(b1), bit(b2), 1 - bit(b3)
            mine = D.at[k, ch, 4 * m1 + 2 * m2 + n3]
            arrived(R2.at[k, ch], rr.at[ST2, k, ring])
            loaded(O3.at[k, slot], ld.at[2, k, slot])
            add_into(mine, O3.at[k, slot], mine, R1.at[k, ch, 2 * m2 + n3], R2.at[k, ch, n3])
            remote(mine, R3.at[k, ch], snd.at[ST3, k], rr.at[ST3, k, ring], flip(me, b3)).start()

    def give(k, ch, stage, blocks, to):
        l, rows = where(ch)
        recv = a0r.at[k] if stage == AG0 else rr.at[stage, k, lax.rem(ch, RING)]
        for j in blocks:
            part = wo[k].at[l, j, rows]
            remote(part, part, snd.at[stage, k], recv, to).start()

    def update(ch):
        l, rows = where(ch)
        slot, ring = lax.rem(ch, 2), lax.rem(ch, RING)
        for k in range(3):
            b1, b2, b3 = AXES[k]
            m1, m2, m3 = bit(b1), bit(b2), bit(b3)
            arrived(R3.at[k, ch], rr.at[ST3, k, ring])
            loaded(O4.at[k, slot], ld.at[3, k, slot])
            loaded(W.at[k, slot], ld.at[4, k, slot])
            total = O4[k, slot].astype(F32)
            for one in (D.at[k, ch, 4 * m1 + 2 * m2 + m3], R1.at[k, ch, 2 * m2 + m3], R2.at[k, ch, m3], R3.at[k, ch]):
                total = total + one[...].astype(F32)
            grad = total.astype(BF16).astype(F32)
            new_m = 0.9 * mo[k][l, rows] + 0.1 * grad
            new_v = 0.95 * vo[k][l, rows] + 0.05 * grad * grad
            old = W[k, slot].astype(F32)
            mo[k][l, rows] = new_m
            vo[k][l, rows] = new_v
            wo[k][l, me, rows] = (old - 0.02 * (new_m * lax.rsqrt(new_v + 1e-8) + 0.1 * old)).astype(BF16)
            give(k, ch, AG3, (me,), flip(me, b3))
            give(k, ch, AG0, (me,), mate)

    def double3(ch):
        l, rows = where(ch)
        for k in range(3):
            b1, b2, b3 = AXES[k]
            got = flip(me, b3)
            arrived(wo[k].at[l, got, rows], rr.at[AG3, k, lax.rem(ch, RING)])
            give(k, ch, AG2, (me, got), flip(me, b2))
            give(k, ch, AG0, (got,), mate)

    def double2(ch):
        l, rows = where(ch)
        for k in range(3):
            b1, b2, b3 = AXES[k]
            held = (me, flip(me, b3))
            got = tuple(flip(j, b2) for j in held)
            arrived(wo[k].at[l, pl.ds(0, 2), rows], rr.at[AG2, k, lax.rem(ch, RING)])
            give(k, ch, AG1, held + got, flip(me, b1))
            give(k, ch, AG0, got, mate)

    def double1(ch):
        l, rows = where(ch)
        for k in range(3):
            b1, b2, b3 = AXES[k]
            held = (me, flip(me, b3))
            got = tuple(flip(j, b1) for j in held + tuple(flip(j, b2) for j in held))
            arrived(wo[k].at[l, pl.ds(0, 4), rows], rr.at[AG1, k, lax.rem(ch, RING)])
            give(k, ch, AG0, got, mate)

    load_own(0, 0)
    for k in range(3):
        pltpu.make_async_copy(m[k], mo[k], mv.at[0, k]).start()
        pltpu.make_async_copy(v[k], vo[k], mv.at[1, k]).start()

    barrier = pltpu.get_barrier_semaphore()
    for b in (1, 2, 4, 8):
        pl.semaphore_signal(barrier, inc=1, device_id={"dp": flip(me, b)}, device_id_type=MESH)
    pl.semaphore_wait(barrier, 4)

    for ch in range(LEAD):
        send_raw(ch)

    for k in range(3):
        loaded(mo[k], mv.at[0, k])
        loaded(vo[k], mv.at[1, k])

    def step(s, _):
        def at(lag, do, *args):
            ch = s - lag

            @pl.when((ch >= 0) & (ch < CHUNKS))
            def _():
                do(*args, ch)

        at(-LEAD, send_raw)
        at(-1, load_own, 0)
        at(0, load_own, 1)
        at(1, load_own, 2)
        at(2, load_own, 3)
        at(0, stage1)
        at(1, stage2)
        at(2, stage3)
        at(3, update)
        at(4, double3)
        at(5, double2)
        at(6, double1)
        return 0

    lax.fori_loop(0, CHUNKS + 6, step, 0)

    for k in range(3):
        arrived(wo[k].at[:, pl.ds(0, 8)], a0r.at[k])
        for stage, sent in (
            (ST0, D.at[k]),
            (ST1, R1.at[k]),
            (ST2, R2.at[k]),
            (ST3, R3.at[k]),
            (AG3, wo[k].at[:, pl.ds(0, 1)]),
            (AG2, wo[k].at[:, pl.ds(0, 2)]),
            (AG1, wo[k].at[:, pl.ds(0, 4)]),
            (AG0, wo[k].at[:, pl.ds(0, 8)]),
        ):
            remote(sent, sent, snd.at[stage, k], a0r.at[k], mate).wait_send()


def write_out(*refs):
    moments, new_w, *targets, sem = refs
    sources = [new_w.at[k] for k in range(3)] + [moments.at[i, k] for i in range(2) for k in range(3)]
    copies = [pltpu.make_async_copy(one, other, sem.at[i]) for i, (one, other) in enumerate(zip(sources, targets, strict=True))]
    for copy in copies:
        copy.start()
    for copy in copies:
        copy.wait()


def tiled(a, parts):
    rows, columns = a.shape[1] // parts // 8, a.shape[2] // 128
    a = a.reshape(LAYERS, parts, rows, 8, columns, 128).transpose(0, 1, 2, 4, 3, 5)
    return a.reshape(LAYERS, parts, TILES, 16, 128)


def untiled(a, shape):
    rows, columns = shape[1] // a.shape[1] // 8, shape[2] // 128
    a = a.reshape(LAYERS, a.shape[1], rows, columns, 8, 128).transpose(0, 1, 2, 4, 3, 5)
    return a.reshape(shape)


def solution(mesh):
    def step(*arrays):
        terms, weights, m, v = (arrays[i : i + 3] for i in (0, 3, 6, 9))
        whole, part = (LAYERS, N, TILES, 16, 128), (LAYERS, TILES, 16, 128)
        block = (T, 16, 128)
        dma = pltpu.SemaphoreType.DMA
        new = pl.pallas_call(
            kernel,
            out_shape=[VM((2, 3, *part), F32), VM((3, *whole), BF16)],
            in_specs=[pl.BlockSpec(memory_space=pltpu.HBM)] * 12,
            out_specs=[pl.BlockSpec(memory_space=pltpu.VMEM)] * 2,
            scratch_shapes=[
                pltpu.VMEM((3, CHUNKS, 8, *block), BF16),
                pltpu.VMEM((3, CHUNKS, 4, *block), BF16),
                pltpu.VMEM((3, CHUNKS, 2, *block), BF16),
                pltpu.VMEM((3, CHUNKS, *block), BF16),
                pltpu.VMEM((3, 2, 4, *block), BF16),
                pltpu.VMEM((3, 2, 2, *block), BF16),
                pltpu.VMEM((3, 2, *block), BF16),
                pltpu.VMEM((3, 2, *block), BF16),
                pltpu.VMEM((3, 2, *block), BF16),
                dma((3, RING0)),
                dma((6, 3, RING)),
                dma((3,)),
                dma((8, 3)),
                dma((5, 3, 2)),
                dma((2, 3)),
            ],
            compiler_params=pltpu.CompilerParams(collective_id=0, has_side_effects=True, vmem_limit_bytes=28 * 2**20),
            name="sum_step_gather",
        )(
            *(tiled(t[0], N) for t in terms),
            *(tiled(one, N) for one in weights),
            *(tiled(one, 1)[:, 0] for one in (*m, *v)),
        )
        new = pl.pallas_call(
            write_out,
            out_shape=[jax.ShapeDtypeStruct(whole, BF16)] * 3 + [jax.ShapeDtypeStruct(part, F32)] * 6,
            in_specs=[pl.BlockSpec(memory_space=pltpu.VMEM)] * 2,
            out_specs=[pl.BlockSpec(memory_space=pltpu.HBM)] * 9,
            scratch_shapes=[dma((9,))],
            compiler_params=pltpu.CompilerParams(vmem_limit_bytes=2**20),
            name="write_out",
        )(*new)
        return (
            *(untiled(one, w.shape) for one, w in zip(new[:3], weights, strict=True)),
            *(untiled(one[:, None], old.shape) for one, old in zip(new[3:], (*m, *v), strict=True)),
        )

    all_of, cut = P(None, None, None), P(None, "dp", None)
    return jax.shard_map(
        step,
        mesh=mesh,
        in_specs=(P(("rep", "dp"), None, None, None),) * 3 + (all_of,) * 3 + (cut,) * 6,
        out_specs=(P("rep", None, None),) * 3 + (P("rep", "dp", None),) * 6,
        check_vma=False,
    )
```

```python
import functools

import jax
import jax.numpy as jnp
from jax import lax
from jax.experimental import pallas as pl
from jax.experimental.pallas import tpu as pltpu
from jax.sharding import PartitionSpec as P

MESH = pl.DeviceIdType.MESH
F32, BF16 = jnp.float32, jnp.bfloat16
N = 16
LAYERS = 2
TILES = 70
AXES = ((8, 4, 2), (4, 2, 8), (2, 8, 4))
SUB = 10
T = TILES // SUB
CHUNKS = LAYERS * SUB
TAIL = 4
LEAD = 2
RING0 = 2 * LEAD + 2
LAG = 2
RING = 6
VM = pltpu.VMEM
ST1, ST2, ST3, AG3, AG2, AG1, ST0, AG0 = range(8)


def add_into(dst, *srcs):
    total = srcs[0][...].astype(F32)
    for one in srcs[1:]:
        total = total + one[...].astype(F32)
    dst[...] = total.astype(BF16)


def kernel(*refs):
    g, w, m, v = (refs[i : i + 3] for i in range(0, 12, 3))
    moments, new_w = refs[12:14]
    ici, mate_part = refs[14:17], refs[17]
    wo = [new_w.at[k] for k in range(3)]
    mo, vo = ([moments.at[i, k] for k in range(3)] for i in range(2))
    D, R1, R2, R3, O1, O2, O3, O4, W, s0r, rr, a0r, snd, ld, mv = refs[18:]
    me = lax.axis_index("dp")

    def bit(b):
        return lax.rem(me // b, 2)

    def flip(i, b):
        return i + b - 2 * b * bit(b)

    core = bit(1)
    mate = flip(me, 1)

    def remote(src, dst, send, recv, to):
        return pltpu.make_async_remote_copy(src, dst, send, recv, device_id={"dp": to}, device_id_type=MESH)

    def arrived(ref, sem):
        remote(ref, ref, snd.at[ST0, 0], sem, mate).wait_recv()

    def loaded(ref, sem):
        pltpu.make_async_copy(ref, ref, sem).wait()

    def where(ch):
        return ch // SUB, pl.ds(lax.rem(ch, SUB) * T, T)

    def owner(k, e1, e2, e3, c):
        b1, b2, b3 = AXES[k]
        return e1 * b1 + e2 * b2 + e3 * b3 + c

    def send_raw(ch):
        l, rows = where(ch)
        for k in range(3):
            for p in range(8):
                j = owner(k, p // 4, p // 2 % 2, p % 2, 1 - core)
                remote(g[k].at[l, j, rows], D.at[k, ch, p], snd.at[ST0, k], s0r.at[k, lax.rem(ch, RING0)], mate).start()

    def load_own(which, ch):
        l, rows = where(ch)
        slot = lax.rem(ch, 2)
        for k in range(3):
            b1, b2, b3 = AXES[k]
            m1, m2, m3 = bit(b1), bit(b2), bit(b3)
            if which == 0:
                for q in range(4):
                    j = owner(k, 1 - m1, q // 2, q % 2, core)
                    pltpu.make_async_copy(g[k].at[l, j, rows], O1.at[k, slot, q], ld.at[0, k, slot]).start()
            elif which == 1:
                for q in range(2):
                    j = owner(k, m1, 1 - m2, q, core)
                    pltpu.make_async_copy(g[k].at[l, j, rows], O2.at[k, slot, q], ld.at[1, k, slot]).start()
            elif which == 2:
                j = owner(k, m1, m2, 1 - m3, core)
                pltpu.make_async_copy(g[k].at[l, j, rows], O3.at[k, slot], ld.at[2, k, slot]).start()
            else:
                pltpu.make_async_copy(g[k].at[l, me, rows], O4.at[k, slot], ld.at[3, k, slot]).start()
                pltpu.make_async_copy(w[k].at[l, me, rows], W.at[k, slot], ld.at[4, k, slot]).start()

    def stage1(ch):
        slot = lax.rem(ch, 2)
        for k in range(3):
            b1, b2, b3 = AXES[k]
            base = 4 * (1 - bit(b1))
            arrived(D.at[k, ch], s0r.at[k, lax.rem(ch, RING0)])
            loaded(O1.at[k, slot], ld.at[0, k, slot])

            def one(q, _):
                add_into(D.at[k, ch, base + q], O1.at[k, slot, q], D.at[k, ch, base + q])
                return 0

            lax.fori_loop(0, 4, one, 0)
            remote(D.at[k, ch, pl.ds(base, 4)], R1.at[k, ch], snd.at[ST1, k], rr.at[ST1, k, lax.rem(ch, RING)], flip(me, b1)).start()

    def stage2(ch):
        slot, ring = lax.rem(ch, 2), lax.rem(ch, RING)
        for k in range(3):
            b1, b2, b3 = AXES[k]
            half = 2 * (1 - bit(b2))
            base = 4 * bit(b1) + half
            arrived(R1.at[k, ch], rr.at[ST1, k, ring])
            loaded(O2.at[k, slot], ld.at[1, k, slot])

            def one(q, _):
                add_into(D.at[k, ch, base + q], O2.at[k, slot, q], D.at[k, ch, base + q], R1.at[k, ch, half + q])
                return 0

            lax.fori_loop(0, 2, one, 0)
            remote(D.at[k, ch, pl.ds(base, 2)], R2.at[k, ch], snd.at[ST2, k], rr.at[ST2, k, ring], flip(me, b2)).start()

    def stage3(ch):
        slot, ring = lax.rem(ch, 2), lax.rem(ch, RING)
        for k in range(3):
            b1, b2, b3 = AXES[k]
            m1, m2, n3 = bit(b1), bit(b2), 1 - bit(b3)
            mine = D.at[k, ch, 4 * m1 + 2 * m2 + n3]
            arrived(R2.at[k, ch], rr.at[ST2, k, ring])
            loaded(O3.at[k, slot], ld.at[2, k, slot])
            add_into(mine, O3.at[k, slot], mine, R1.at[k, ch, 2 * m2 + n3], R2.at[k, ch, n3])
            remote(mine, R3.at[k, ch], snd.at[ST3, k], rr.at[ST3, k, ring], flip(me, b3)).start()

    def give(k, ch, stage, blocks, to):
        l, rows = where(ch)
        recv = a0r.at[k] if stage == AG0 else rr.at[stage, k, lax.rem(ch, RING)]
        for j in blocks:
            part = wo[k].at[l, j, rows]
            remote(part, part, snd.at[stage, k], recv, to).start()

    def update(ch):
        l, rows = where(ch)
        slot, ring = lax.rem(ch, 2), lax.rem(ch, RING)

        @pl.when(ch == 0)
        def _():
            for k in range(3):
                loaded(mo[k], mv.at[0, k])
                loaded(vo[k], mv.at[1, k])

        for k in range(3):
            b1, b2, b3 = AXES[k]
            m1, m2, m3 = bit(b1), bit(b2), bit(b3)
            arrived(R3.at[k, ch], rr.at[ST3, k, ring])
            loaded(O4.at[k, slot], ld.at[3, k, slot])
            loaded(W.at[k, slot], ld.at[4, k, slot])
            total = O4[k, slot].astype(F32)
            for one in (D.at[k, ch, 4 * m1 + 2 * m2 + m3], R1.at[k, ch, 2 * m2 + m3], R2.at[k, ch, m3], R3.at[k, ch]):
                total = total + one[...].astype(F32)
            grad = total.astype(BF16).astype(F32)
            new_m = 0.9 * mo[k][l, rows] + 0.1 * grad
            new_v = 0.95 * vo[k][l, rows] + 0.05 * grad * grad
            old = W[k, slot].astype(F32)
            mo[k][l, rows] = new_m
            vo[k][l, rows] = new_v
            wo[k][l, me, rows] = (old - 0.02 * (new_m * lax.rsqrt(new_v + 1e-8) + 0.1 * old)).astype(BF16)
            give(k, ch, AG3, (me,), flip(me, b3))
            give(k, ch, AG0, (me,), mate)

    def double3(ch):
        l, rows = where(ch)
        for k in range(3):
            b1, b2, b3 = AXES[k]
            got = flip(me, b3)
            arrived(wo[k].at[l, got, rows], rr.at[AG3, k, lax.rem(ch, RING)])
            give(k, ch, AG2, (me, got), flip(me, b2))
            give(k, ch, AG0, (got,), mate)

    def double2(ch):
        l, rows = where(ch)
        for k in range(3):
            b1, b2, b3 = AXES[k]
            held = (me, flip(me, b3))
            got = tuple(flip(j, b2) for j in held)
            arrived(wo[k].at[l, pl.ds(0, 2), rows], rr.at[AG2, k, lax.rem(ch, RING)])
            give(k, ch, AG0, got, mate)

            @pl.when(ch >= TAIL)
            def _():
                give(k, ch, AG1, held + got, flip(me, b1))

            @pl.when(ch < TAIL)
            def _():
                for q in range(4):
                    ici[k][q, rows] = wo[k][l, owner(k, bit(b1), q // 2, q % 2, core), rows]

    def double1(ch):
        l, rows = where(ch)
        for k in range(3):
            b1, b2, b3 = AXES[k]
            held = (me, flip(me, b3))
            got = tuple(flip(j, b1) for j in held + tuple(flip(j, b2) for j in held))
            arrived(wo[k].at[l, pl.ds(0, 4), rows], rr.at[AG1, k, lax.rem(ch, RING)])

            @pl.when(ch < CHUNKS - 1)
            def _():
                give(k, ch, AG0, got, mate)

            @pl.when(ch == CHUNKS - 1)
            def _():
                for q in range(4):
                    mate_part[k, q] = wo[k][l, owner(k, 1 - bit(b1), q // 2, q % 2, core), rows]

    load_own(0, 0)
    for k in range(3):
        pltpu.make_async_copy(m[k], mo[k], mv.at[0, k]).start()
        pltpu.make_async_copy(v[k], vo[k], mv.at[1, k]).start()

    barrier = pltpu.get_barrier_semaphore()
    for b in (1, 2, 4, 8):
        pl.semaphore_signal(barrier, inc=1, device_id={"dp": flip(me, b)}, device_id_type=MESH)
    pl.semaphore_wait(barrier, 4)

    for ch in range(LEAD):
        send_raw(ch)

    def step(s, _):
        def at(lag, do, *args, start=0):
            ch = s - lag

            @pl.when((ch >= start) & (ch < CHUNKS))
            def _():
                do(*args, ch)

        at(0, stage1)
        at(-LEAD, send_raw)
        at(-1, load_own, 0)
        at(LAG - 1, load_own, 1)
        at(LAG, load_own, 2)
        at(LAG + 1, load_own, 3)
        at(LAG, stage2)
        at(LAG + 1, stage3)
        at(LAG + 2, update)
        at(LAG + 3, double3)
        at(LAG + 4, double2)
        at(LAG + 5, double1, start=TAIL)
        return 0

    lax.fori_loop(0, CHUNKS + LAG + 5, step, 0)

    for k in range(3):
        arrived(D.at[k, :, pl.ds(0, 7)], a0r.at[k])
        for stage, sent in (
            (ST0, D.at[k]),
            (ST1, R1.at[k]),
            (ST2, R2.at[k]),
            (ST3, R3.at[k]),
            (AG3, wo[k].at[:, pl.ds(0, 1)]),
            (AG2, wo[k].at[:, pl.ds(0, 2)]),
            (AG1, R1.at[k, pl.ds(0, CHUNKS - TAIL)]),
            (AG0, D.at[k, :, pl.ds(0, 7)]),
        ):
            remote(sent, sent, snd.at[stage, k], a0r.at[k], mate).wait_send()


def run_copies(pairs, sem):
    copies = [pltpu.make_async_copy(one, other, sem.at[i]) for i, (one, other) in enumerate(pairs)]
    for copy in copies:
        copy.start()
    for copy in copies:
        copy.wait()


def far_blocks(k):
    me = lax.axis_index("dp")
    b1, b2, b3 = AXES[k]
    near = lax.rem(me // b1, 2)
    core = lax.rem(me, 2)
    spots = [q // 2 * b2 + q % 2 * b3 for q in range(4)]
    return [[e * b1 + spot + c for spot in spots] for e, c in ((1 - near, core), (1 - near, 1 - core), (near, core), (near, 1 - core))]


def write_early(moments, new_w, *refs):
    *targets, sem = refs
    late = pl.ds(0, TAIL * T)
    pairs = []
    for k in range(3):
        rest = pl.ds(TAIL * T, TILES - TAIL * T)
        pairs += [(new_w.at[k, 1], targets[k].at[1]), (new_w.at[k, 0, :, rest], targets[k].at[0, :, rest])]
        for blocks in far_blocks(k)[2:]:
            pairs += [(new_w.at[k, 0, j, late], targets[k].at[0, j, late]) for j in blocks]
    pairs += [(moments.at[i, k], targets[3 + 3 * i + k]) for i in range(2) for k in range(3)]
    run_copies(pairs, sem)


def write_next(*refs):
    link, targets, sem = refs[0:3], refs[6:9], refs[9]
    late = pl.ds(0, TAIL * T)
    pairs = []
    for k in range(3):
        pairs += [(link[k].at[q], targets[k].at[0, j, late]) for q, j in enumerate(far_blocks(k)[0])]
    run_copies(pairs, sem)


def write_last(*refs):
    mates, last, targets, sem = refs[0:3], refs[3], refs[7:10], refs[10]
    late, end = pl.ds(0, TAIL * T), pl.ds(TILES - T, T)
    pairs = []
    for k in range(3):
        for q, j in enumerate(far_blocks(k)[1]):
            pairs.append((mates[k].at[q], targets[k].at[0, j, late]))
            pairs.append((last.at[k, q], targets[k].at[1, j, end]))
    run_copies(pairs, sem)


def tiled(a, parts):
    rows, columns = a.shape[1] // parts // 8, a.shape[2] // 128
    a = a.reshape(LAYERS, parts, rows, 8, columns, 128).transpose(0, 1, 2, 4, 3, 5)
    return a.reshape(LAYERS, parts, TILES, 16, 128)


def untiled(a, shape):
    rows, columns = shape[1] // a.shape[1] // 8, shape[2] // 128
    a = a.reshape(LAYERS, a.shape[1], rows, columns, 8, 128).transpose(0, 1, 2, 4, 3, 5)
    return a.reshape(shape)


def solution(mesh):
    def step(*arrays):
        terms, weights, m, v = (arrays[i : i + 3] for i in (0, 3, 6, 9))
        whole, part = (LAYERS, N, TILES, 16, 128), (LAYERS, TILES, 16, 128)
        block = (T, 16, 128)
        dma = pltpu.SemaphoreType.DMA
        new = pl.pallas_call(
            kernel,
            out_shape=[VM((2, 3, *part), F32), VM((3, *whole), BF16)] + [VM((4, TAIL * T, 16, 128), BF16)] * 3 + [VM((3, 4, *block), BF16)],
            in_specs=[pl.BlockSpec(memory_space=pltpu.HBM)] * 12,
            out_specs=[pl.BlockSpec(memory_space=pltpu.VMEM)] * 6,
            scratch_shapes=[
                pltpu.VMEM((3, CHUNKS, 8, *block), BF16),
                pltpu.VMEM((3, CHUNKS, 4, *block), BF16),
                pltpu.VMEM((3, CHUNKS, 2, *block), BF16),
                pltpu.VMEM((3, CHUNKS, *block), BF16),
                pltpu.VMEM((3, 2, 4, *block), BF16),
                pltpu.VMEM((3, 2, 2, *block), BF16),
                pltpu.VMEM((3, 2, *block), BF16),
                pltpu.VMEM((3, 2, *block), BF16),
                pltpu.VMEM((3, 2, *block), BF16),
                dma((3, RING0)),
                dma((6, 3, RING)),
                dma((3,)),
                dma((8, 3)),
                dma((5, 3, 2)),
                dma((2, 3)),
            ],
            compiler_params=pltpu.CompilerParams(collective_id=0, has_side_effects=True, vmem_limit_bytes=28 * 2**20),
            name="sum_step_gather",
        )(
            *(tiled(t[0], N) for t in terms),
            *(tiled(one, N) for one in weights),
            *(tiled(one, 1)[:, 0] for one in (*m, *v)),
        )
        moments, new_w, *sent, last = new
        hbm, any_space, vmem = (pl.BlockSpec(memory_space=one) for one in (pltpu.HBM, pl.ANY, pltpu.VMEM))
        out_w, out_m = [jax.ShapeDtypeStruct(whole, BF16)] * 3, [jax.ShapeDtypeStruct(part, F32)] * 6

        def plain(body, out_shape, in_specs, copies, aliases, flops):
            return pl.pallas_call(
                body,
                out_shape=out_shape,
                in_specs=in_specs,
                out_specs=[hbm] * len(out_shape),
                scratch_shapes=[dma((copies,))],
                input_output_aliases=aliases,
                compiler_params=pltpu.CompilerParams(vmem_limit_bytes=2**20),
                cost_estimate=pl.CostEstimate(flops=flops, bytes_accessed=flops // 100, transcendentals=0),
                name=body.__name__,
            )

        link = [lax.ppermute(one, "dp", [(i, i ^ AXES[k][0]) for i in range(N)]) for k, one in enumerate(sent)]
        *new_w, m0, m1, m2, v0, v1, v2 = plain(write_early, out_w + out_m, [vmem] * 2, 36, {}, 2 * 10**9)(moments, new_w)
        *new_w, link0, link1, link2, last = lax.optimization_barrier((*new_w, *link, last))
        link = (link0, link1, link2)
        mates = [lax.ppermute(one, "dp", [(i, i ^ 1) for i in range(N)]) for one in (*link, last)]
        new_w = plain(write_next, out_w, [any_space] * 3 + [hbm] * 3, 12, {3: 0, 4: 1, 5: 2}, 10**9)(*link, *new_w)
        new_w = plain(write_last, out_w, [any_space] * 4 + [hbm] * 3, 24, {4: 0, 5: 1, 6: 2}, 10**9)(*mates, *new_w)
        new = (*new_w, m0, m1, m2, v0, v1, v2)
        return (
            *(untiled(one, w.shape) for one, w in zip(new[:3], weights, strict=True)),
            *(untiled(one[:, None], old.shape) for one, old in zip(new[3:], (*m, *v), strict=True)),
        )

    all_of, cut = P(None, None, None), P(None, "dp", None)
    return jax.shard_map(
        step,
        mesh=mesh,
        in_specs=(P(("rep", "dp"), None, None, None),) * 3 + (all_of,) * 3 + (cut,) * 6,
        out_specs=(P("rep", None, None),) * 3 + (P("rep", "dp", None),) * 6,
        check_vma=False,
    )
```

```python
import jax
import jax.numpy as jnp
from jax import lax
from jax.experimental import pallas as pl
from jax.experimental.pallas import tpu as pltpu
from jax.sharding import PartitionSpec as P


MESH = pl.DeviceIdType.MESH
F32, BF16 = jnp.float32, jnp.bfloat16
N = 16
LAYERS = 2
TILES = 70
AXES = ((8, 4, 2), (4, 2, 8), (2, 8, 4))
SUB = 10
T = TILES // SUB
CHUNKS = LAYERS * SUB
TAIL = 4
LEAD = 2
LAG = 2
RING0 = 2 * LEAD + 2 + LAG
RING = 6
VM = pltpu.VMEM
ST1, ST2, ST3, AG3, AG2, AG1, ST0, AG0 = range(8)


def add_into(dst, *srcs):
    total = srcs[0][...].astype(F32)
    for one in srcs[1:]:
        total = total + one[...].astype(F32)
    dst[...] = total.astype(BF16)


def kernel(*refs):
    g, w, m, v = (refs[i : i + 3] for i in range(0, 12, 3))
    moments, new_w = refs[12:14]
    split, both, mate_part = refs[14:17]
    wo = [new_w.at[k] for k in range(3)]
    mo, vo = ([moments.at[i, k] for k in range(3)] for i in range(2))
    D, R1, R2, R3, O1, O2, O3, O4, W, s0r, rr, a0r, snd, ld, mv = refs[17:]
    me = lax.axis_index("dp")

    def bit(b):
        return lax.rem(me // b, 2)

    def flip(i, b):
        return i + b - 2 * b * bit(b)

    core = bit(1)
    mate = flip(me, 1)

    def remote(src, dst, send, recv, to):
        return pltpu.make_async_remote_copy(src, dst, send, recv, device_id={"dp": to}, device_id_type=MESH)

    def arrived(ref, sem):
        remote(ref, ref, snd.at[ST0, 0], sem, mate).wait_recv()

    def loaded(ref, sem):
        pltpu.make_async_copy(ref, ref, sem).wait()

    def where(ch):
        return ch // SUB, pl.ds(lax.rem(ch, SUB) * T, T)

    def owner(k, e1, e2, e3, c):
        b1, b2, b3 = AXES[k]
        return e1 * b1 + e2 * b2 + e3 * b3 + c

    def send_raw(ch):
        l, rows = where(ch)
        for half in range(2):
            for k in range(3):
                side = bit(AXES[k][0]) if half else 1 - bit(AXES[k][0])
                for q in range(4):
                    j = owner(k, side, q // 2, q % 2, 1 - core)
                    remote(g[k].at[l, j, rows], D.at[k, ch, 4 * side + q], snd.at[ST0, k], s0r.at[half, k, lax.rem(ch, RING0)], mate).start()

    def load_own(which, ch):
        l, rows = where(ch)
        slot = lax.rem(ch, 2)
        for k in range(3):
            b1, b2, b3 = AXES[k]
            m1, m2, m3 = bit(b1), bit(b2), bit(b3)
            if which == 0:
                for q in range(4):
                    j = owner(k, 1 - m1, q // 2, q % 2, core)
                    pltpu.make_async_copy(g[k].at[l, j, rows], O1.at[k, slot, q], ld.at[0, k, slot]).start()
            elif which == 1:
                for q in range(2):
                    j = owner(k, m1, 1 - m2, q, core)
                    pltpu.make_async_copy(g[k].at[l, j, rows], O2.at[k, slot, q], ld.at[1, k, slot]).start()
            elif which == 2:
                j = owner(k, m1, m2, 1 - m3, core)
                pltpu.make_async_copy(g[k].at[l, j, rows], O3.at[k, slot], ld.at[2, k, slot]).start()
            else:
                pltpu.make_async_copy(g[k].at[l, me, rows], O4.at[k, slot], ld.at[3, k, slot]).start()
                pltpu.make_async_copy(w[k].at[l, me, rows], W.at[k, slot], ld.at[4, k, slot]).start()

    def stage1(ch):
        slot = lax.rem(ch, 2)
        for k in range(3):
            b1, _, _ = AXES[k]
            base = 4 * (1 - bit(b1))
            arrived(D.at[k, ch, pl.ds(base, 4)], s0r.at[0, k, lax.rem(ch, RING0)])
            loaded(O1.at[k, slot], ld.at[0, k, slot])

            def one(q, _):
                add_into(D.at[k, ch, base + q], O1.at[k, slot, q], D.at[k, ch, base + q])
                return 0

            lax.fori_loop(0, 4, one, 0)
            remote(D.at[k, ch, pl.ds(base, 4)], R1.at[k, ch], snd.at[ST1, k], rr.at[ST1, k, lax.rem(ch, RING)], flip(me, b1)).start()

    def stage2(ch):
        slot, ring = lax.rem(ch, 2), lax.rem(ch, RING)
        for k in range(3):
            b1, b2, _ = AXES[k]
            half = 2 * (1 - bit(b2))
            base = 4 * bit(b1) + half
            arrived(D.at[k, ch, pl.ds(4 * bit(b1), 4)], s0r.at[1, k, lax.rem(ch, RING0)])
            arrived(R1.at[k, ch], rr.at[ST1, k, ring])
            loaded(O2.at[k, slot], ld.at[1, k, slot])

            def one(q, _):
                add_into(D.at[k, ch, base + q], O2.at[k, slot, q], D.at[k, ch, base + q], R1.at[k, ch, half + q])
                return 0

            lax.fori_loop(0, 2, one, 0)
            remote(D.at[k, ch, pl.ds(base, 2)], R2.at[k, ch], snd.at[ST2, k], rr.at[ST2, k, ring], flip(me, b2)).start()

    def stage3(ch):
        slot, ring = lax.rem(ch, 2), lax.rem(ch, RING)
        for k in range(3):
            b1, b2, b3 = AXES[k]
            m1, m2, n3 = bit(b1), bit(b2), 1 - bit(b3)
            mine = D.at[k, ch, 4 * m1 + 2 * m2 + n3]
            arrived(R2.at[k, ch], rr.at[ST2, k, ring])
            loaded(O3.at[k, slot], ld.at[2, k, slot])
            add_into(mine, O3.at[k, slot], mine, R1.at[k, ch, 2 * m2 + n3], R2.at[k, ch, n3])
            remote(mine, R3.at[k, ch], snd.at[ST3, k], rr.at[ST3, k, ring], flip(me, b3)).start()

    def give(k, ch, stage, blocks, to):
        l, rows = where(ch)
        recv = a0r.at[k, lax.min(ch // TAIL, 1)] if stage == AG0 else rr.at[stage, k, lax.rem(ch, RING)]
        for j in blocks:
            part = wo[k].at[l, j, rows]
            remote(part, part, snd.at[stage, k], recv, to).start()

    def update(ch):
        l, rows = where(ch)
        slot, ring = lax.rem(ch, 2), lax.rem(ch, RING)

        @pl.when(ch == 0)
        def _():
            for k in range(3):
                loaded(mo[k], mv.at[0, k])
                loaded(vo[k], mv.at[1, k])

        for k in range(3):
            b1, b2, b3 = AXES[k]
            m1, m2, m3 = bit(b1), bit(b2), bit(b3)
            arrived(R3.at[k, ch], rr.at[ST3, k, ring])
            loaded(O4.at[k, slot], ld.at[3, k, slot])
            loaded(W.at[k, slot], ld.at[4, k, slot])
            total = O4[k, slot].astype(F32)
            for one in (D.at[k, ch, 4 * m1 + 2 * m2 + m3], R1.at[k, ch, 2 * m2 + m3], R2.at[k, ch, m3], R3.at[k, ch]):
                total = total + one[...].astype(F32)
            grad = total.astype(BF16).astype(F32)
            new_m = 0.9 * mo[k][l, rows] + 0.1 * grad
            new_v = 0.95 * vo[k][l, rows] + 0.05 * grad * grad
            old = W[k, slot].astype(F32)
            mo[k][l, rows] = new_m
            vo[k][l, rows] = new_v
            wo[k][l, me, rows] = (old - 0.02 * (new_m * lax.rsqrt(new_v + 1e-8) + 0.1 * old)).astype(BF16)
            give(k, ch, AG3, (me,), flip(me, b3))
            give(k, ch, AG0, (me,), mate)

    def double3(ch):
        l, rows = where(ch)
        for k in range(3):
            _, b2, b3 = AXES[k]
            got = flip(me, b3)
            arrived(wo[k].at[l, got, rows], rr.at[AG3, k, lax.rem(ch, RING)])
            give(k, ch, AG2, (me, got), flip(me, b2))
            give(k, ch, AG0, (got,), mate)

    def double2(ch):
        l, rows = where(ch)
        for k in range(3):
            b1, b2, b3 = AXES[k]
            held = (me, flip(me, b3))
            got = tuple(flip(j, b2) for j in held)
            arrived(wo[k].at[l, pl.ds(0, 2), rows], rr.at[AG2, k, lax.rem(ch, RING)])
            give(k, ch, AG0, got, mate)

            @pl.when(ch >= TAIL)
            def _():
                give(k, ch, AG1, held + got, flip(me, b1))


    def double1(ch):
        l, rows = where(ch)
        for k in range(3):
            b1, b2, b3 = AXES[k]
            held = (me, flip(me, b3))
            got = tuple(flip(j, b1) for j in held + tuple(flip(j, b2) for j in held))
            arrived(wo[k].at[l, pl.ds(0, 4), rows], rr.at[AG1, k, lax.rem(ch, RING)])

            @pl.when(ch < CHUNKS - 1)
            def _():
                give(k, ch, AG0, got, mate)

            @pl.when(ch == CHUNKS - 1)
            def _():
                for q in range(4):
                    mate_part[k, q] = wo[k][l, owner(k, 1 - bit(b1), q // 2, q % 2, core), rows]

    def take_late():
        late = pl.ds(0, TAIL * T)
        for k in range(3):
            arrived(R1.at[k, pl.ds(0, TAIL)], a0r.at[k, 0])

            @pl.when(core == k - 1 if k else core >= 0)
            def _():
                def one(q, _):
                    if k:
                        split[q] = wo[k][0, owner(k, bit(AXES[k][0]), q // 4, lax.rem(q // 2, 2), lax.rem(q, 2)), late]
                    else:
                        both[q] = wo[k][0, owner(k, bit(AXES[k][0]), q // 2, lax.rem(q, 2), core), late]
                    return 0

                lax.fori_loop(0, 8 if k else 4, one, 0)

    load_own(0, 0)
    for k in range(3):
        pltpu.make_async_copy(m[k], mo[k], mv.at[0, k]).start()
        pltpu.make_async_copy(v[k], vo[k], mv.at[1, k]).start()

    barrier = pltpu.get_barrier_semaphore()
    for b in (1, 2, 4, 8):
        pl.semaphore_signal(barrier, inc=1, device_id={"dp": flip(me, b)}, device_id_type=MESH)
    pl.semaphore_wait(barrier, 4)

    for ch in range(LEAD):
        send_raw(ch)

    def step(s, _):
        def at(lag, do, *args, start=0):
            ch = s - lag

            @pl.when((ch >= start) & (ch < CHUNKS))
            def _():
                do(*args, ch)

        at(0, stage1)
        at(-LEAD, send_raw)
        at(-1, load_own, 0)
        at(LAG - 1, load_own, 1)
        at(LAG, load_own, 2)
        at(LAG + 1, load_own, 3)
        at(LAG, stage2)
        at(LAG + 1, stage3)
        at(LAG + 2, update)
        at(LAG + 3, double3)
        at(LAG + 4, double2)
        at(LAG + 5, double1, start=TAIL)
        pl.when(s == CHUNKS)(take_late)
        return 0

    lax.fori_loop(0, CHUNKS + LAG + 5, step, 0)

    for k in range(3):
        arrived(wo[k].at[:, pl.ds(0, 7), pl.ds(0, 62)], a0r.at[k, 1])

    for k in range(3):
        for stage, sent in (
            (ST0, D.at[k]),
            (ST1, R1.at[k]),
            (ST2, R2.at[k]),
            (ST3, R3.at[k]),
            (AG3, wo[k].at[:, pl.ds(0, 1)]),
            (AG2, wo[k].at[:, pl.ds(0, 2)]),
            (AG1, R1.at[k, pl.ds(0, CHUNKS - TAIL)]),
            (AG0, D.at[k, :, pl.ds(0, 7)]),
        ):
            remote(sent, sent, snd.at[stage, k], a0r.at[k, 0], mate).wait_send()


def run_copies(pairs, sem):
    copies = [pltpu.make_async_copy(one, other, sem.at[i]) for i, (one, other) in enumerate(pairs)]
    for copy in copies:
        copy.start()
    for copy in copies:
        copy.wait()


def late_blocks(k, far):
    b1, b2, b3 = AXES[k]
    side = lax.rem(lax.axis_index("dp") // b1, 2)
    side = 1 - side if far else side
    return [side * b1 + q // 4 * b2 + q // 2 % 2 * b3 + q % 2 for q in range(8)]


def write_early(moments, new_w, *refs):
    *targets, sem = refs
    late = pl.ds(0, TAIL * T)
    pairs = []
    for k in range(3):
        rest = pl.ds(TAIL * T, TILES - TAIL * T)
        pairs += [(new_w.at[k, 1], targets[k].at[1]), (new_w.at[k, 0, :, rest], targets[k].at[0, :, rest])]
        pairs += [(new_w.at[k, 0, j, late], targets[k].at[0, j, late]) for j in late_blocks(k, False)]
    pairs += [(moments.at[i, k], targets[3 + 3 * i + k]) for i in range(2) for k in range(3)]
    run_copies(pairs, sem)


def put_late(split, both, targets, core, other, sem, more=()):
    late = pl.ds(0, TAIL * T)
    far = late_blocks(0, True)
    pairs = [*more] + [(both.at[q], targets[0].at[0, far[2 * q] + other, late]) for q in range(4)]
    for k in (1, 2):

        @pl.when(core == k - 1)
        def _():
            run_copies(pairs + [(split.at[q], targets[k].at[0, j, late]) for q, j in enumerate(late_blocks(k, True))], sem)


def write_next(*refs):
    split, both, targets, sem = refs[0], refs[1], refs[5:8], refs[8]
    core = lax.rem(lax.axis_index("dp"), 2)
    put_late(split, both, targets, core, core, sem)


def write_last(*refs):
    split, both, last, targets, sem = refs[0], refs[1], refs[2], refs[6:9], refs[9]
    core = lax.rem(lax.axis_index("dp"), 2)
    end, more = pl.ds(TILES - T, T), []
    for k in range(3):
        far = late_blocks(k, True)
        more += [(last.at[k, q], targets[k].at[1, far[2 * q] + 1 - core, end]) for q in range(4)]
    put_late(split, both, targets, 1 - core, 1 - core, sem, more)


def tiled(a, parts):
    rows, columns = a.shape[1] // parts // 8, a.shape[2] // 128
    a = a.reshape(LAYERS, parts, rows, 8, columns, 128).transpose(0, 1, 2, 4, 3, 5)
    return a.reshape(LAYERS, parts, TILES, 16, 128)


def untiled(a, shape):
    rows, columns = shape[1] // a.shape[1] // 8, shape[2] // 128
    a = a.reshape(LAYERS, a.shape[1], rows, columns, 8, 128).transpose(0, 1, 2, 4, 3, 5)
    return a.reshape(shape)


def solution(mesh):
    def step(*arrays):
        terms, weights, m, v = (arrays[i : i + 3] for i in (0, 3, 6, 9))
        whole, part = (LAYERS, N, TILES, 16, 128), (LAYERS, TILES, 16, 128)
        block = (T, 16, 128)
        dma = pltpu.SemaphoreType.DMA
        new = pl.pallas_call(
            kernel,
            out_shape=[VM((2, 3, *part), F32), VM((3, *whole), BF16)] + [VM((8, TAIL * T, 16, 128), BF16), VM((4, TAIL * T, 16, 128), BF16), VM((3, 4, *block), BF16)],
            in_specs=[pl.BlockSpec(memory_space=pltpu.HBM)] * 12,
            out_specs=[pl.BlockSpec(memory_space=pltpu.VMEM)] * 5,
            scratch_shapes=[
                pltpu.VMEM((3, CHUNKS, 8, *block), BF16),
                pltpu.VMEM((3, CHUNKS, 4, *block), BF16),
                pltpu.VMEM((3, CHUNKS, 2, *block), BF16),
                pltpu.VMEM((3, CHUNKS, *block), BF16),
                pltpu.VMEM((3, 2, 4, *block), BF16),
                pltpu.VMEM((3, 2, 2, *block), BF16),
                pltpu.VMEM((3, 2, *block), BF16),
                pltpu.VMEM((3, 2, *block), BF16),
                pltpu.VMEM((3, 2, *block), BF16),
                dma((2, 3, RING0)),
                dma((6, 3, RING)),
                dma((3, 2)),
                dma((8, 3)),
                dma((5, 3, 2)),
                dma((2, 3)),
            ],
            compiler_params=pltpu.CompilerParams(collective_id=0, has_side_effects=True, vmem_limit_bytes=28 * 2**20),
            name="sum_step_gather",
        )(
            *(tiled(t[0], N) for t in terms),
            *(tiled(one, N) for one in weights),
            *(tiled(one, 1)[:, 0] for one in (*m, *v)),
        )
        moments, new_w, split, both, last = new
        hbm, any_space, vmem = (pl.BlockSpec(memory_space=one) for one in (pltpu.HBM, pl.ANY, pltpu.VMEM))
        out_w, out_m = [jax.ShapeDtypeStruct(whole, BF16)] * 3, [jax.ShapeDtypeStruct(part, F32)] * 6

        def plain(body, out_shape, in_specs, copies, aliases, flops):
            return pl.pallas_call(
                body,
                out_shape=out_shape,
                in_specs=in_specs,
                out_specs=[hbm] * len(out_shape),
                scratch_shapes=[dma((copies,))],
                input_output_aliases=aliases,
                compiler_params=pltpu.CompilerParams(vmem_limit_bytes=2**20),
                cost_estimate=pl.CostEstimate(flops=flops, bytes_accessed=flops // 100, transcendentals=0),
            )

        split = lax.ppermute(split, "dp", [(i, i ^ (AXES[2][0] if i % 2 else AXES[1][0])) for i in range(N)])
        both = lax.ppermute(both, "dp", [(i, i ^ AXES[0][0]) for i in range(N)])
        last = lax.ppermute(last, "dp", [(i, i ^ 1) for i in range(N)])
        *new_w, m0, m1, m2, v0, v1, v2 = plain(write_early, out_w + out_m, [vmem] * 2, 36, {}, 2 * 10**9)(moments, new_w)
        *new_w, split, both = lax.optimization_barrier((*new_w, split, both))
        mates = [lax.ppermute(one, "dp", [(i, i ^ 1) for i in range(N)]) for one in (split, both)]
        new_w = plain(write_next, out_w, [any_space] * 2 + [hbm] * 3, 12, {2: 0, 3: 1, 4: 2}, 10**9)(split, both, *new_w)
        new_w = plain(write_last, out_w, [any_space] * 3 + [hbm] * 3, 24, {3: 0, 4: 1, 5: 2}, 10**9)(*mates, last, *new_w)
        new = (*new_w, m0, m1, m2, v0, v1, v2)
        return (
            *(untiled(one, w.shape) for one, w in zip(new[:3], weights, strict=True)),
            *(untiled(one[:, None], old.shape) for one, old in zip(new[3:], (*m, *v), strict=True)),
        )

    all_of, cut = P(None, None, None), P(None, "dp", None)
    return jax.shard_map(
        step,
        mesh=mesh,
        in_specs=(P(("rep", "dp"), None, None, None),) * 3 + (all_of,) * 3 + (cut,) * 6,
        out_specs=(P("rep", None, None),) * 3 + (P("rep", "dp", None),) * 6,
        check_vma=False,
    )
```

```python
import jax
import jax.numpy as jnp
from jax import lax
from jax.experimental import pallas as pl
from jax.experimental.pallas import tpu as pltpu
from jax.sharding import PartitionSpec as P


MESH = pl.DeviceIdType.MESH
F32, BF16 = jnp.float32, jnp.bfloat16
N = 16
LAYERS = 2
TILES = 70
AXES = ((8, 4, 2), (4, 2, 8), (2, 8, 4))
SUB = 10
T = TILES // SUB
CHUNKS = LAYERS * SUB
TAIL = 4
LEAD = 1
LAG = 1
RING = 4
VM = pltpu.VMEM
ST1, ST2, ST3, AG3, AG2, AG1, ST0, AG0 = range(8)


def add_into(dst, *srcs):
    total = srcs[0][...].astype(F32)
    for one in srcs[1:]:
        total = total + one[...].astype(F32)
    dst[...] = total.astype(BF16)


def kernel(*refs):
    g, w, m, v = (refs[i : i + 3] for i in range(0, 12, 3))
    moments, new_w = refs[12:14]
    split, both, mate_part = refs[14:17]
    wo = [new_w.at[k] for k in range(3)]
    mo, vo = ([moments.at[i, k] for k in range(3)] for i in range(2))
    D, R1, R2, R3, O1, O2, O3, O4, W, s0r, rr, a0r, snd, ld, mv = refs[17:]
    me = lax.axis_index("dp")

    def bit(b):
        return lax.rem(me // b, 2)

    def flip(i, b):
        return i + b - 2 * b * bit(b)

    core = bit(1)
    mate = flip(me, 1)

    def remote(src, dst, send, recv, to):
        return pltpu.make_async_remote_copy(src, dst, send, recv, device_id={"dp": to}, device_id_type=MESH)

    def arrived(ref, sem):
        remote(ref, ref, snd.at[ST0], sem, mate).wait_recv()

    def loaded(ref, sem):
        pltpu.make_async_copy(ref, ref, sem).wait()

    def where(ch):
        return ch // SUB, pl.ds(lax.rem(ch, SUB) * T, T)

    def owner(k, e1, e2, e3, c):
        b1, b2, b3 = AXES[k]
        return e1 * b1 + e2 * b2 + e3 * b3 + c

    def send_raw(ch):
        l, rows = where(ch)
        for half in range(2):
            for k in range(3):
                side = bit(AXES[k][0]) if half else 1 - bit(AXES[k][0])
                for q in range(4):
                    j = owner(k, side, q // 2, q % 2, 1 - core)
                    sem = s0r.at[3 if half else k, lax.rem(ch, RING)]
                    remote(g[k].at[l, j, rows], D.at[k, ch, 4 * side + q], snd.at[ST0], sem, mate).start()

    def load_own(which, ch):
        l, rows = where(ch)
        slot = lax.rem(ch, 2)
        for k in range(3):
            b1, b2, b3 = AXES[k]
            m1, m2, m3 = bit(b1), bit(b2), bit(b3)
            if which == 0:
                for q in range(4):
                    j = owner(k, 1 - m1, q // 2, q % 2, core)
                    pltpu.make_async_copy(g[k].at[l, j, rows], O1.at[slot, k, q], ld.at[0, slot]).start()
            elif which == 1:
                for q in range(2):
                    j = owner(k, m1, 1 - m2, q, core)
                    pltpu.make_async_copy(g[k].at[l, j, rows], O2.at[slot, k, q], ld.at[1, slot]).start()
            elif which == 2:
                j = owner(k, m1, m2, 1 - m3, core)
                pltpu.make_async_copy(g[k].at[l, j, rows], O3.at[slot, k], ld.at[2, slot]).start()
            else:
                pltpu.make_async_copy(g[k].at[l, me, rows], O4.at[slot, k], ld.at[3, slot]).start()
                pltpu.make_async_copy(w[k].at[l, me, rows], W.at[slot, k], ld.at[4, slot]).start()

    def stage1(ch):
        slot, ring = lax.rem(ch, 2), lax.rem(ch, RING)
        loaded(O1.at[slot], ld.at[0, slot])
        for k in range(3):
            b1, _, _ = AXES[k]
            base = 4 * (1 - bit(b1))
            arrived(D.at[k, ch, pl.ds(base, 4)], s0r.at[k, ring])

            def one(q, _):
                add_into(D.at[k, ch, base + q], O1.at[slot, k, q], D.at[k, ch, base + q])
                return 0

            lax.fori_loop(0, 4, one, 0)
            remote(D.at[k, ch, pl.ds(base, 4)], R1.at[ch, k], snd.at[ST1], rr.at[ST1, ring], flip(me, b1)).start()

    def stage2(ch):
        slot, ring = lax.rem(ch, 2), lax.rem(ch, RING)
        arrived(R1.at[ch], s0r.at[3, ring])
        arrived(R1.at[ch], rr.at[ST1, ring])
        loaded(O2.at[slot], ld.at[1, slot])
        for k in range(3):
            b1, b2, _ = AXES[k]
            half = 2 * (1 - bit(b2))
            base = 4 * bit(b1) + half

            def one(q, _):
                add_into(D.at[k, ch, base + q], O2.at[slot, k, q], D.at[k, ch, base + q], R1.at[ch, k, half + q])
                return 0

            lax.fori_loop(0, 2, one, 0)
            remote(D.at[k, ch, pl.ds(base, 2)], R2.at[ch, k], snd.at[ST2], rr.at[ST2, ring], flip(me, b2)).start()

    def stage3(ch):
        slot, ring = lax.rem(ch, 2), lax.rem(ch, RING)
        arrived(R2.at[ch], rr.at[ST2, ring])
        loaded(O3.at[slot], ld.at[2, slot])
        for k in range(3):
            b1, b2, b3 = AXES[k]
            m1, m2, n3 = bit(b1), bit(b2), 1 - bit(b3)
            mine = D.at[k, ch, 4 * m1 + 2 * m2 + n3]
            add_into(mine, O3.at[slot, k], mine, R1.at[ch, k, 2 * m2 + n3], R2.at[ch, k, n3])
            remote(mine, R3.at[ch, k], snd.at[ST3], rr.at[ST3, ring], flip(me, b3)).start()

    def give(k, ch, stage, blocks, to):
        l, rows = where(ch)
        recv = a0r.at[lax.min(ch // TAIL, 1)] if stage == AG0 else rr.at[stage, lax.rem(ch, RING)]
        for j in blocks:
            part = wo[k].at[l, j, rows]
            remote(part, part, snd.at[stage], recv, to).start()

    def update(ch):
        l, rows = where(ch)
        slot, ring = lax.rem(ch, 2), lax.rem(ch, RING)

        @pl.when(ch == 0)
        def _():
            loaded(moments, mv.at[0])

        arrived(R3.at[ch], rr.at[ST3, ring])
        loaded(O4.at[slot], ld.at[3, slot])
        loaded(W.at[slot], ld.at[4, slot])
        for k in range(3):
            b1, b2, b3 = AXES[k]
            m1, m2, m3 = bit(b1), bit(b2), bit(b3)
            total = O4[slot, k].astype(F32)
            for one in (D.at[k, ch, 4 * m1 + 2 * m2 + m3], R1.at[ch, k, 2 * m2 + m3], R2.at[ch, k, m3], R3.at[ch, k]):
                total = total + one[...].astype(F32)
            grad = total.astype(BF16).astype(F32)
            new_m = 0.9 * mo[k][l, rows] + 0.1 * grad
            new_v = 0.95 * vo[k][l, rows] + 0.05 * grad * grad
            old = W[slot, k].astype(F32)
            mo[k][l, rows] = new_m
            vo[k][l, rows] = new_v
            wo[k][l, me, rows] = (old - 0.02 * (new_m * lax.rsqrt(new_v + 1e-8) + 0.1 * old)).astype(BF16)
            give(k, ch, AG3, (me,), flip(me, b3))
            give(k, ch, AG0, (me,), mate)

    def double3(ch):
        arrived(R3.at[ch], rr.at[AG3, lax.rem(ch, RING)])
        for k in range(3):
            _, b2, b3 = AXES[k]
            got = flip(me, b3)
            give(k, ch, AG2, (me, got), flip(me, b2))
            give(k, ch, AG0, (got,), mate)

    def double2(ch):
        arrived(R2.at[ch], rr.at[AG2, lax.rem(ch, RING)])
        for k in range(3):
            b1, b2, b3 = AXES[k]
            held = (me, flip(me, b3))
            got = tuple(flip(j, b2) for j in held)
            give(k, ch, AG0, got, mate)

            @pl.when(ch >= TAIL)
            def _():
                give(k, ch, AG1, held + got, flip(me, b1))


    def double1(ch):
        l, rows = where(ch)
        arrived(R1.at[ch], rr.at[AG1, lax.rem(ch, RING)])
        for k in range(3):
            b1, b2, b3 = AXES[k]
            held = (me, flip(me, b3))
            got = tuple(flip(j, b1) for j in held + tuple(flip(j, b2) for j in held))

            @pl.when(ch < CHUNKS - 1)
            def _():
                give(k, ch, AG0, got, mate)

            @pl.when(ch == CHUNKS - 1)
            def _():
                for q in range(4):
                    mate_part[k, q] = wo[k][l, owner(k, 1 - bit(b1), q // 2, q % 2, core), rows]

    def take_late():
        late = pl.ds(0, TAIL * T)
        arrived(R1.at[pl.ds(0, TAIL)], a0r.at[0])
        for k in range(3):

            @pl.when(core == k - 1 if k else core >= 0)
            def _():
                def one(q, _):
                    if k:
                        split[q] = wo[k][0, owner(k, bit(AXES[k][0]), q // 4, lax.rem(q // 2, 2), lax.rem(q, 2)), late]
                    else:
                        both[q] = wo[k][0, owner(k, bit(AXES[k][0]), q // 2, lax.rem(q, 2), core), late]
                    return 0

                lax.fori_loop(0, 8 if k else 4, one, 0)

    load_own(0, 0)
    for k in range(3):
        pltpu.make_async_copy(m[k], mo[k], mv.at[0]).start()
        pltpu.make_async_copy(v[k], vo[k], mv.at[0]).start()

    barrier = pltpu.get_barrier_semaphore()
    for b in (1, 2, 4, 8):
        pl.semaphore_signal(barrier, inc=1, device_id={"dp": flip(me, b)}, device_id_type=MESH)
    pl.semaphore_wait(barrier, 4)

    for ch in range(LEAD):
        send_raw(ch)

    def step(s, _):
        def at(lag, do, *args, start=0):
            ch = s - lag

            @pl.when((ch >= start) & (ch < CHUNKS))
            def _():
                do(*args, ch)

        at(0, stage1)
        at(-LEAD, send_raw)
        at(-1, load_own, 0)
        at(LAG - 1, load_own, 1)
        at(LAG, load_own, 2)
        at(LAG + 1, load_own, 3)
        at(LAG, stage2)
        at(LAG + 1, stage3)
        at(LAG + 2, update)
        at(LAG + 3, double3)
        at(LAG + 4, double2)
        at(LAG + 5, double1, start=TAIL)
        pl.when(s == CHUNKS)(take_late)
        return 0

    lax.fori_loop(0, CHUNKS + LAG + 5, step, 0)

    arrived(new_w.at[:, :, pl.ds(0, 7), pl.ds(0, 62)], a0r.at[1])
    for stage, sent in (
        (ST0, D),
        (ST1, R1),
        (ST2, R2),
        (ST3, R3),
        (AG3, R3),
        (AG2, R2),
        (AG1, R1.at[pl.ds(0, CHUNKS - TAIL)]),
        (AG0, D.at[:, :, pl.ds(0, 7)]),
    ):
        remote(sent, sent, snd.at[stage], a0r.at[0], mate).wait_send()


def run_copies(groups, sem):
    for i, (pairs, _) in enumerate(groups):
        for one, other in pairs:
            pltpu.make_async_copy(one, other, sem.at[i]).start()
    for i, (_, total) in enumerate(groups):
        pltpu.make_async_copy(total, total, sem.at[i]).wait()


def late_blocks(k, far):
    b1, b2, b3 = AXES[k]
    side = lax.rem(lax.axis_index("dp") // b1, 2)
    side = 1 - side if far else side
    return [side * b1 + q // 4 * b2 + q // 2 % 2 * b3 + q % 2 for q in range(8)]


def write_early(moments, new_w, *refs):
    *targets, sem = refs
    late, rest = pl.ds(0, TAIL * T), pl.ds(TAIL * T, TILES - TAIL * T)
    pairs = []
    for k in range(3):
        pairs += [(new_w.at[k, 1], targets[k].at[1]), (new_w.at[k, 0, :, rest], targets[k].at[0, :, rest])]
        pairs += [(new_w.at[k, 0, j, late], targets[k].at[0, j, late]) for j in late_blocks(k, False)]
    small = [(moments.at[i, k], targets[3 + 3 * i + k]) for i in range(2) for k in range(3)]
    run_copies([(pairs, new_w.at[:, :, :, pl.ds(0, TILES - TAIL * T // 4)]), (small, moments)], sem)


def put_late(split, both, targets, core, sem, more=()):
    late = pl.ds(0, TAIL * T)
    far = late_blocks(0, True)
    shared = ([(both.at[q], targets[0].at[0, far[2 * q] + core, late]) for q in range(4)], both)
    for k in (1, 2):

        @pl.when(core == k - 1)
        def _():
            run_copies([*more, shared, ([(split.at[q], targets[k].at[0, j, late]) for q, j in enumerate(late_blocks(k, True))], split)], sem)


def write_next(*refs):
    split, both, targets, sem = refs[0], refs[1], refs[5:8], refs[8]
    put_late(split, both, targets, lax.rem(lax.axis_index("dp"), 2), sem)


def write_last(*refs):
    split, both, last, targets, sem = refs[0], refs[1], refs[2], refs[6:9], refs[9]
    other = 1 - lax.rem(lax.axis_index("dp"), 2)
    end, ends = pl.ds(TILES - T, T), []
    for k in range(3):
        far = late_blocks(k, True)
        ends += [(last.at[k, q], targets[k].at[1, far[2 * q] + other, end]) for q in range(4)]
    put_late(split, both, targets, other, sem, [(ends, last)])


def tiled(a, parts):
    rows, columns = a.shape[1] // parts // 8, a.shape[2] // 128
    a = a.reshape(LAYERS, parts, rows, 8, columns, 128).transpose(0, 1, 2, 4, 3, 5)
    return a.reshape(LAYERS, parts, TILES, 16, 128)


def untiled(a, shape):
    rows, columns = shape[1] // a.shape[1] // 8, shape[2] // 128
    a = a.reshape(LAYERS, a.shape[1], rows, columns, 8, 128).transpose(0, 1, 2, 4, 3, 5)
    return a.reshape(shape)


def solution(mesh):
    def step(*arrays):
        terms, weights, m, v = (arrays[i : i + 3] for i in (0, 3, 6, 9))
        whole, part = (LAYERS, N, TILES, 16, 128), (LAYERS, TILES, 16, 128)
        block = (T, 16, 128)
        dma = pltpu.SemaphoreType.DMA
        new = pl.pallas_call(
            kernel,
            out_shape=[VM((2, 3, *part), F32), VM((3, *whole), BF16)] + [VM((8, TAIL * T, 16, 128), BF16), VM((4, TAIL * T, 16, 128), BF16), VM((3, 4, *block), BF16)],
            in_specs=[pl.BlockSpec(memory_space=pltpu.HBM)] * 12,
            out_specs=[pl.BlockSpec(memory_space=pltpu.VMEM)] * 5,
            scratch_shapes=[
                pltpu.VMEM((3, CHUNKS, 8, *block), BF16),
                pltpu.VMEM((CHUNKS, 3, 4, *block), BF16),
                pltpu.VMEM((CHUNKS, 3, 2, *block), BF16),
                pltpu.VMEM((CHUNKS, 3, *block), BF16),
                pltpu.VMEM((2, 3, 4, *block), BF16),
                pltpu.VMEM((2, 3, 2, *block), BF16),
                pltpu.VMEM((2, 3, *block), BF16),
                pltpu.VMEM((2, 3, *block), BF16),
                pltpu.VMEM((2, 3, *block), BF16),
                dma((4, RING)),
                dma((6, RING)),
                dma((2,)),
                dma((8,)),
                dma((5, 2)),
                dma((1,)),
            ],
            compiler_params=pltpu.CompilerParams(collective_id=0, has_side_effects=True, vmem_limit_bytes=28 * 2**20),
            name="sum_step_gather",
        )(
            *(tiled(t[0], N) for t in terms),
            *(tiled(one, N) for one in weights),
            *(tiled(one, 1)[:, 0] for one in (*m, *v)),
        )
        moments, new_w, split, both, last = new
        hbm, any_space, vmem = (pl.BlockSpec(memory_space=one) for one in (pltpu.HBM, pl.ANY, pltpu.VMEM))
        out_w, out_m = [jax.ShapeDtypeStruct(whole, BF16)] * 3, [jax.ShapeDtypeStruct(part, F32)] * 6

        def plain(body, out_shape, in_specs, semaphores, aliases, flops):
            return pl.pallas_call(
                body,
                out_shape=out_shape,
                in_specs=in_specs,
                out_specs=[hbm] * len(out_shape),
                scratch_shapes=[dma((semaphores,))],
                input_output_aliases=aliases,
                compiler_params=pltpu.CompilerParams(vmem_limit_bytes=2**20),
                cost_estimate=pl.CostEstimate(flops=flops, bytes_accessed=flops // 100, transcendentals=0),
            )

        split = lax.ppermute(split, "dp", [(i, i ^ (AXES[2][0] if i % 2 else AXES[1][0])) for i in range(N)])
        both = lax.ppermute(both, "dp", [(i, i ^ AXES[0][0]) for i in range(N)])
        last = lax.ppermute(last, "dp", [(i, i ^ 1) for i in range(N)])
        *new_w, m0, m1, m2, v0, v1, v2 = plain(write_early, out_w + out_m, [vmem] * 2, 2, {}, 2 * 10**9)(moments, new_w)
        *new_w, split, both = lax.optimization_barrier((*new_w, split, both))
        mates = [lax.ppermute(one, "dp", [(i, i ^ 1) for i in range(N)]) for one in (split, both)]
        new_w = plain(write_next, out_w, [any_space] * 2 + [hbm] * 3, 2, {2: 0, 3: 1, 4: 2}, 10**9)(split, both, *new_w)
        new_w = plain(write_last, out_w, [any_space] * 3 + [hbm] * 3, 3, {3: 0, 4: 1, 5: 2}, 10**9)(*mates, last, *new_w)
        new = (*new_w, m0, m1, m2, v0, v1, v2)
        return (
            *(untiled(one, w.shape) for one, w in zip(new[:3], weights, strict=True)),
            *(untiled(one[:, None], old.shape) for one, old in zip(new[3:], (*m, *v), strict=True)),
        )

    all_of, cut = P(None, None, None), P(None, "dp", None)
    return jax.shard_map(
        step,
        mesh=mesh,
        in_specs=(P(("rep", "dp"), None, None, None),) * 3 + (all_of,) * 3 + (cut,) * 6,
        out_specs=(P("rep", None, None),) * 3 + (P("rep", "dp", None),) * 6,
        check_vma=False,
    )
```

```python
import jax
import jax.numpy as jnp
from jax import lax
from jax.experimental import pallas as pl
from jax.experimental.pallas import tpu as pltpu
from jax.sharding import PartitionSpec as P


MESH = pl.DeviceIdType.MESH
F32, BF16 = jnp.float32, jnp.bfloat16
N = 16
LAYERS = 2
TILES = 70
AXES = ((8, 4, 2), (4, 2, 8), (2, 8, 4))
SUB = 10
T = TILES // SUB
CHUNKS = LAYERS * SUB
TAIL = 4
PIECES = (pl.ds(0, 2), pl.ds(2, T - 2))
LEAD = 2
LAG = 2
RING = 6
RING0 = 8
VM = pltpu.VMEM
ST1, ST2, ST3, AG3, AG2, AG1, ST0, AG0 = range(8)


def add_into(dst, *srcs):
    total = srcs[0][...].astype(F32)
    for one in srcs[1:]:
        total = total + one[...].astype(F32)
    dst[...] = total.astype(BF16)


def kernel(*refs):
    g, w, m, v = (refs[i : i + 3] for i in range(0, 12, 3))
    moments, new_w = refs[12:14]
    split, both, mate_part = refs[14:17]
    wo = [new_w.at[k] for k in range(3)]
    mo, vo = ([moments.at[i, k] for k in range(3)] for i in range(2))
    D, R1, R2, R3, O1, O2, O3, O4, W, s0r, rr, a0r, snd, ld, mv = refs[17:]
    me = lax.axis_index("dp")

    def bit(b):
        return lax.rem(me // b, 2)

    def flip(i, b):
        return i + b - 2 * b * bit(b)

    core = bit(1)
    mate = flip(me, 1)

    def remote(src, dst, send, recv, to):
        return pltpu.make_async_remote_copy(src, dst, send, recv, device_id={"dp": to}, device_id_type=MESH)

    def arrived(ref, sem):
        remote(ref, ref, snd.at[ST0], sem, mate).wait_recv()

    def loaded(ref, sem):
        pltpu.make_async_copy(ref, ref, sem).wait()

    def where(ch):
        return ch // SUB, pl.ds(lax.rem(ch, SUB) * T, T)

    def owner(k, e1, e2, e3, c):
        b1, b2, b3 = AXES[k]
        return e1 * b1 + e2 * b2 + e3 * b3 + c

    def send_raw(ch, halves=(0, 1)):
        l, rows = where(ch)
        for half in halves:
            for k in range(3):
                side = bit(AXES[k][0]) if half else 1 - bit(AXES[k][0])
                for q in range(4):
                    j = owner(k, side, q // 2, q % 2, 1 - core)
                    sem = s0r.at[3 if half else k, lax.rem(ch, RING0)]
                    remote(g[k].at[l, j, rows], D.at[k, ch, 4 * side + q], snd.at[ST0], sem, mate).start()

    def send_first():
        for piece, rows in enumerate(PIECES):
            for k in range(3):
                side = 1 - bit(AXES[k][0])
                sem = s0r.at[k, 0 if piece else RING0 - 1]
                for q in range(4):
                    j = owner(k, side, q // 2, q % 2, 1 - core)
                    remote(g[k].at[0, j, rows], D.at[k, 0, 4 * side + q, rows], snd.at[ST0], sem, mate).start()

    def stage1_first():
        loaded(O1.at[0], ld.at[0, 0])
        for piece, rows in enumerate(PIECES):
            for k in range(3):
                b1 = AXES[k][0]
                base = 4 * (1 - bit(b1))
                part = D.at[k, 0, pl.ds(base, 4), rows]
                arrived(part, s0r.at[k, 0 if piece else RING0 - 1])
                for q in range(4):
                    add_into(D.at[k, 0, base + q, rows], O1.at[0, k, q, rows], D.at[k, 0, base + q, rows])
                remote(part, R1.at[0, k, :, rows], snd.at[ST1], rr.at[ST1, 0], flip(me, b1)).start()

    def load_own(which, ch):
        l, rows = where(ch)
        slot = lax.rem(ch, 2)
        for k in range(3):
            b1, b2, b3 = AXES[k]
            m1, m2, m3 = bit(b1), bit(b2), bit(b3)
            if which == 0:
                for q in range(4):
                    j = owner(k, 1 - m1, q // 2, q % 2, core)
                    pltpu.make_async_copy(g[k].at[l, j, rows], O1.at[slot, k, q], ld.at[0, slot]).start()
            elif which == 1:
                for q in range(2):
                    j = owner(k, m1, 1 - m2, q, core)
                    pltpu.make_async_copy(g[k].at[l, j, rows], O2.at[slot, k, q], ld.at[1, slot]).start()
            elif which == 2:
                j = owner(k, m1, m2, 1 - m3, core)
                pltpu.make_async_copy(g[k].at[l, j, rows], O3.at[slot, k], ld.at[2, slot]).start()
            else:
                pltpu.make_async_copy(g[k].at[l, me, rows], O4.at[slot, k], ld.at[3, slot]).start()
                pltpu.make_async_copy(w[k].at[l, me, rows], W.at[slot, k], ld.at[4, slot]).start()

    def stage1(ch):
        slot, ring = lax.rem(ch, 2), lax.rem(ch, RING)
        loaded(O1.at[slot], ld.at[0, slot])
        for k in range(3):
            b1, _, _ = AXES[k]
            base = 4 * (1 - bit(b1))
            arrived(D.at[k, ch, pl.ds(base, 4)], s0r.at[k, lax.rem(ch, RING0)])

            def one(q, _):
                add_into(D.at[k, ch, base + q], O1.at[slot, k, q], D.at[k, ch, base + q])
                return 0

            lax.fori_loop(0, 4, one, 0)
            remote(D.at[k, ch, pl.ds(base, 4)], R1.at[ch, k], snd.at[ST1], rr.at[ST1, ring], flip(me, b1)).start()

    def stage2(ch):
        slot, ring = lax.rem(ch, 2), lax.rem(ch, RING)
        arrived(R1.at[ch], s0r.at[3, lax.rem(ch, RING0)])
        arrived(R1.at[ch], rr.at[ST1, ring])
        loaded(O2.at[slot], ld.at[1, slot])
        for k in range(3):
            b1, b2, _ = AXES[k]
            half = 2 * (1 - bit(b2))
            base = 4 * bit(b1) + half

            def one(q, _):
                add_into(D.at[k, ch, base + q], O2.at[slot, k, q], D.at[k, ch, base + q], R1.at[ch, k, half + q])
                return 0

            lax.fori_loop(0, 2, one, 0)
            remote(D.at[k, ch, pl.ds(base, 2)], R2.at[ch, k], snd.at[ST2], rr.at[ST2, ring], flip(me, b2)).start()

    def stage3(ch):
        slot, ring = lax.rem(ch, 2), lax.rem(ch, RING)
        arrived(R2.at[ch], rr.at[ST2, ring])
        loaded(O3.at[slot], ld.at[2, slot])
        for k in range(3):
            b1, b2, b3 = AXES[k]
            m1, m2, n3 = bit(b1), bit(b2), 1 - bit(b3)
            mine = D.at[k, ch, 4 * m1 + 2 * m2 + n3]
            add_into(mine, O3.at[slot, k], mine, R1.at[ch, k, 2 * m2 + n3], R2.at[ch, k, n3])
            remote(mine, R3.at[ch, k], snd.at[ST3], rr.at[ST3, ring], flip(me, b3)).start()

    def give(k, ch, stage, blocks, to):
        l, rows = where(ch)
        recv = a0r.at[lax.min(ch // TAIL, 1)] if stage == AG0 else rr.at[stage, lax.rem(ch, RING)]
        for j in blocks:
            part = wo[k].at[l, j, rows]
            remote(part, part, snd.at[stage], recv, to).start()

    def update(ch):
        l, rows = where(ch)
        slot, ring = lax.rem(ch, 2), lax.rem(ch, RING)

        @pl.when(ch == 0)
        def _():
            loaded(moments, mv.at[0])

        arrived(R3.at[ch], rr.at[ST3, ring])
        loaded(O4.at[slot], ld.at[3, slot])
        loaded(W.at[slot], ld.at[4, slot])
        for k in range(3):
            b1, b2, b3 = AXES[k]
            m1, m2, m3 = bit(b1), bit(b2), bit(b3)
            total = O4[slot, k].astype(F32)
            for one in (D.at[k, ch, 4 * m1 + 2 * m2 + m3], R1.at[ch, k, 2 * m2 + m3], R2.at[ch, k, m3], R3.at[ch, k]):
                total = total + one[...].astype(F32)
            grad = total.astype(BF16).astype(F32)
            new_m = 0.9 * mo[k][l, rows] + 0.1 * grad
            new_v = 0.95 * vo[k][l, rows] + 0.05 * grad * grad
            old = W[slot, k].astype(F32)
            mo[k][l, rows] = new_m
            vo[k][l, rows] = new_v
            wo[k][l, me, rows] = (old - 0.02 * (new_m * lax.rsqrt(new_v + 1e-8) + 0.1 * old)).astype(BF16)
            give(k, ch, AG3, (me,), flip(me, b3))
            give(k, ch, AG0, (me,), mate)

    def double3(ch):
        arrived(R3.at[ch], rr.at[AG3, lax.rem(ch, RING)])
        for k in range(3):
            _, b2, b3 = AXES[k]
            got = flip(me, b3)
            give(k, ch, AG2, (me, got), flip(me, b2))
            give(k, ch, AG0, (got,), mate)

    def double2(ch):
        arrived(R2.at[ch], rr.at[AG2, lax.rem(ch, RING)])
        for k in range(3):
            b1, b2, b3 = AXES[k]
            held = (me, flip(me, b3))
            got = tuple(flip(j, b2) for j in held)
            give(k, ch, AG0, got, mate)

            @pl.when(ch >= TAIL)
            def _():
                give(k, ch, AG1, held + got, flip(me, b1))


    def double1(ch):
        l, rows = where(ch)
        arrived(R1.at[ch], rr.at[AG1, lax.rem(ch, RING)])
        for k in range(3):
            b1, b2, b3 = AXES[k]
            held = (me, flip(me, b3))
            got = tuple(flip(j, b1) for j in held + tuple(flip(j, b2) for j in held))

            @pl.when(ch < CHUNKS - 1)
            def _():
                give(k, ch, AG0, got, mate)

            @pl.when(ch == CHUNKS - 1)
            def _():
                for q in range(4):
                    mate_part[k, q] = wo[k][l, owner(k, 1 - bit(b1), q // 2, q % 2, core), rows]

    def take_late():
        late = pl.ds(0, TAIL * T)
        arrived(R1.at[pl.ds(0, TAIL)], a0r.at[0])
        for k in range(3):

            @pl.when(core == k - 1 if k else core >= 0)
            def _():
                def one(q, _):
                    if k:
                        split[q] = wo[k][0, owner(k, bit(AXES[k][0]), q // 4, lax.rem(q // 2, 2), lax.rem(q, 2)), late]
                    else:
                        both[q] = wo[k][0, owner(k, bit(AXES[k][0]), q // 2, lax.rem(q, 2), core), late]
                    return 0

                lax.fori_loop(0, 8 if k else 4, one, 0)

    load_own(0, 0)
    for k in range(3):
        pltpu.make_async_copy(m[k], mo[k], mv.at[0]).start()
        pltpu.make_async_copy(v[k], vo[k], mv.at[0]).start()

    barrier = pltpu.get_barrier_semaphore()
    for b in (1, 2, 4, 8):
        pl.semaphore_signal(barrier, inc=1, device_id={"dp": flip(me, b)}, device_id_type=MESH)
    pl.semaphore_wait(barrier, 4)

    send_first()
    send_raw(0, (1,))
    send_raw(1)
    stage1_first()
    send_raw(2)

    def step(s, _):
        def at(lag, do, *args, start=0):
            ch = s - lag

            @pl.when((ch >= start) & (ch < CHUNKS))
            def _():
                do(*args, ch)

        at(0, stage1, start=1)
        at(-LEAD, send_raw, start=LEAD + 1)
        at(-1, load_own, 0)
        at(LAG - 1, load_own, 1)
        at(LAG, load_own, 2)
        at(LAG + 1, load_own, 3)
        at(LAG, stage2)
        at(LAG + 1, stage3)
        at(LAG + 2, update)
        at(LAG + 3, double3)
        at(LAG + 4, double2)
        at(LAG + 5, double1, start=TAIL)
        pl.when(s == CHUNKS)(take_late)
        return 0

    lax.fori_loop(0, CHUNKS + LAG + 5, step, 0)

    arrived(new_w.at[:, :, pl.ds(0, 7), pl.ds(0, 62)], a0r.at[1])
    for stage, sent in (
        (ST0, D),
        (ST1, R1),
        (ST2, R2),
        (ST3, R3),
        (AG3, R3),
        (AG2, R2),
        (AG1, R1.at[pl.ds(0, CHUNKS - TAIL)]),
        (AG0, D.at[:, :, pl.ds(0, 7)]),
    ):
        remote(sent, sent, snd.at[stage], a0r.at[0], mate).wait_send()


def run_copies(groups, sem):
    for i, (pairs, _) in enumerate(groups):
        for one, other in pairs:
            pltpu.make_async_copy(one, other, sem.at[i]).start()
    for i, (_, total) in enumerate(groups):
        pltpu.make_async_copy(total, total, sem.at[i]).wait()


def late_blocks(k, far):
    b1, b2, b3 = AXES[k]
    side = lax.rem(lax.axis_index("dp") // b1, 2)
    side = 1 - side if far else side
    return [side * b1 + q // 4 * b2 + q // 2 % 2 * b3 + q % 2 for q in range(8)]


def write_early(moments, new_w, *refs):
    *targets, sem = refs
    late, rest = pl.ds(0, TAIL * T), pl.ds(TAIL * T, TILES - TAIL * T)
    pairs = []
    for k in range(3):
        pairs += [(new_w.at[k, 1], targets[k].at[1]), (new_w.at[k, 0, :, rest], targets[k].at[0, :, rest])]
        pairs += [(new_w.at[k, 0, j, late], targets[k].at[0, j, late]) for j in late_blocks(k, False)]
    small = [(moments.at[i, k], targets[3 + 3 * i + k]) for i in range(2) for k in range(3)]
    run_copies([(pairs, new_w.at[:, :, :, pl.ds(0, TILES - TAIL * T // 4)]), (small, moments)], sem)


def put_late(split, both, targets, core, sem, more=()):
    late = pl.ds(0, TAIL * T)
    far = late_blocks(0, True)
    shared = ([(both.at[q], targets[0].at[0, far[2 * q] + core, late]) for q in range(4)], both)
    for k in (1, 2):

        @pl.when(core == k - 1)
        def _():
            run_copies([*more, shared, ([(split.at[q], targets[k].at[0, j, late]) for q, j in enumerate(late_blocks(k, True))], split)], sem)


def write_next(*refs):
    split, both, last, targets, sem = refs[0], refs[1], refs[2], refs[6:9], refs[9]
    core = lax.rem(lax.axis_index("dp"), 2)
    end, ends = pl.ds(TILES - T, T), []
    for k in range(3):
        far = late_blocks(k, True)
        ends += [(last.at[k, q], targets[k].at[1, far[2 * q] + 1 - core, end]) for q in range(4)]
    put_late(split, both, targets, core, sem, [(ends, last)])


def write_last(*refs):
    split, both, targets, sem = refs[0], refs[1], refs[5:8], refs[8]
    put_late(split, both, targets, 1 - lax.rem(lax.axis_index("dp"), 2), sem)


def tiled(a, parts):
    rows, columns = a.shape[1] // parts // 8, a.shape[2] // 128
    a = a.reshape(LAYERS, parts, rows, 8, columns, 128).transpose(0, 1, 2, 4, 3, 5)
    return a.reshape(LAYERS, parts, TILES, 16, 128)


def untiled(a, shape):
    rows, columns = shape[1] // a.shape[1] // 8, shape[2] // 128
    a = a.reshape(LAYERS, a.shape[1], rows, columns, 8, 128).transpose(0, 1, 2, 4, 3, 5)
    return a.reshape(shape)


def solution(mesh):
    def step(*arrays):
        terms, weights, m, v = (arrays[i : i + 3] for i in (0, 3, 6, 9))
        whole, part = (LAYERS, N, TILES, 16, 128), (LAYERS, TILES, 16, 128)
        block = (T, 16, 128)
        dma = pltpu.SemaphoreType.DMA
        new = pl.pallas_call(
            kernel,
            out_shape=[VM((2, 3, *part), F32), VM((3, *whole), BF16)] + [VM((8, TAIL * T, 16, 128), BF16), VM((4, TAIL * T, 16, 128), BF16), VM((3, 4, *block), BF16)],
            in_specs=[pl.BlockSpec(memory_space=pltpu.HBM)] * 12,
            out_specs=[pl.BlockSpec(memory_space=pltpu.VMEM)] * 5,
            scratch_shapes=[
                pltpu.VMEM((3, CHUNKS, 8, *block), BF16),
                pltpu.VMEM((CHUNKS, 3, 4, *block), BF16),
                pltpu.VMEM((CHUNKS, 3, 2, *block), BF16),
                pltpu.VMEM((CHUNKS, 3, *block), BF16),
                pltpu.VMEM((2, 3, 4, *block), BF16),
                pltpu.VMEM((2, 3, 2, *block), BF16),
                pltpu.VMEM((2, 3, *block), BF16),
                pltpu.VMEM((2, 3, *block), BF16),
                pltpu.VMEM((2, 3, *block), BF16),
                dma((4, RING0)),
                dma((6, RING)),
                dma((2,)),
                dma((8,)),
                dma((5, 2)),
                dma((1,)),
            ],
            compiler_params=pltpu.CompilerParams(collective_id=0, has_side_effects=True, vmem_limit_bytes=28 * 2**20),
            name="sum_step_gather",
        )(
            *(tiled(t[0], N) for t in terms),
            *(tiled(one, N) for one in weights),
            *(tiled(one, 1)[:, 0] for one in (*m, *v)),
        )
        moments, new_w, split, both, last = new
        hbm, any_space, vmem = (pl.BlockSpec(memory_space=one) for one in (pltpu.HBM, pl.ANY, pltpu.VMEM))
        out_w, out_m = [jax.ShapeDtypeStruct(whole, BF16)] * 3, [jax.ShapeDtypeStruct(part, F32)] * 6

        def plain(body, out_shape, in_specs, semaphores, aliases, flops):
            return pl.pallas_call(
                body,
                out_shape=out_shape,
                in_specs=in_specs,
                out_specs=[hbm] * len(out_shape),
                scratch_shapes=[dma((semaphores,))],
                input_output_aliases=aliases,
                compiler_params=pltpu.CompilerParams(vmem_limit_bytes=2**20),
                cost_estimate=pl.CostEstimate(flops=flops, bytes_accessed=flops // 100, transcendentals=0),
            )

        split = lax.ppermute(split, "dp", [(i, i ^ (AXES[2][0] if i % 2 else AXES[1][0])) for i in range(N)])
        both = lax.ppermute(both, "dp", [(i, i ^ AXES[0][0]) for i in range(N)])
        last = lax.ppermute(last, "dp", [(i, i ^ 1) for i in range(N)])
        *new_w, m0, m1, m2, v0, v1, v2 = plain(write_early, out_w + out_m, [vmem] * 2, 2, {}, 2 * 10**9)(moments, new_w)
        *new_w, split, both = lax.optimization_barrier((*new_w, split, both))
        mates = [lax.ppermute(one, "dp", [(i, i ^ 1) for i in range(N)]) for one in (split, both)]
        new_w = plain(write_next, out_w, [any_space] * 3 + [hbm] * 3, 3, {3: 0, 4: 1, 5: 2}, 10**9)(split, both, last, *new_w)
        new_w = plain(write_last, out_w, [any_space] * 2 + [hbm] * 3, 2, {2: 0, 3: 1, 4: 2}, 10**9)(*mates, *new_w)
        new = (*new_w, m0, m1, m2, v0, v1, v2)
        return (
            *(untiled(one, w.shape) for one, w in zip(new[:3], weights, strict=True)),
            *(untiled(one[:, None], old.shape) for one, old in zip(new[3:], (*m, *v), strict=True)),
        )

    all_of, cut = P(None, None, None), P(None, "dp", None)
    return jax.shard_map(
        step,
        mesh=mesh,
        in_specs=(P(("rep", "dp"), None, None, None),) * 3 + (all_of,) * 3 + (cut,) * 6,
        out_specs=(P("rep", None, None),) * 3 + (P("rep", "dp", None),) * 6,
        check_vma=False,
    )
```

```python
import jax
import jax.numpy as jnp
from jax import lax
from jax.experimental import pallas as pl
from jax.experimental.pallas import tpu as pltpu
from jax.sharding import PartitionSpec as P


MESH = pl.DeviceIdType.MESH
F32, BF16 = jnp.float32, jnp.bfloat16
N = 16
LAYERS = 2
TILES = 70
AXES = ((8, 4, 2), (4, 2, 8), (2, 8, 4))
SUB = 10
T = TILES // SUB
CHUNKS = LAYERS * SUB
TAIL = 4
PIECES = (pl.ds(0, 2), pl.ds(2, T - 2))
LEAD = 2
LAG = 2
RING, RING1, NEAR = 4, 6, 8
VM = pltpu.VMEM
ST1, ST2, ST3, AG3, AG2, AG1, _, AG0 = range(8)


def add_into(dst, *srcs):
    total = srcs[0][...].astype(F32)
    for one in srcs[1:]:
        total = total + one[...].astype(F32)
    dst[...] = total.astype(BF16)


def kernel(*refs):
    g, w, m, v = (refs[i : i + 3] for i in range(0, 12, 3))
    moments, new_w = refs[12:14]
    split, both, mate_part = refs[14:17]
    wo = [new_w.at[k] for k in range(3)]
    mo, vo = ([moments.at[i, k] for k in range(3)] for i in range(2))
    D, R1, R2, R3, O1, O2, O3, O4, W, far, near, early, rr, a0r, snd, ld, mv = refs[17:]
    me = lax.axis_index("dp")

    def bit(b):
        return lax.rem(me // b, 2)

    def flip(i, b):
        return i + b - 2 * b * bit(b)

    core = bit(1)
    mate = flip(me, 1)

    def remote(src, dst, send, recv, to):
        return pltpu.make_async_remote_copy(src, dst, send, recv, device_id={"dp": to}, device_id_type=MESH)

    def arrived(ref, sem):
        remote(ref, ref, snd.at[0], sem, mate).wait_recv()

    def loaded(ref, sem):
        pltpu.make_async_copy(ref, ref, sem).wait()

    def came(stage, ch):
        return rr.at[lax.rem(ch, RING1) if stage == ST1 else RING1 + RING * (stage - 1) + lax.rem(ch, RING)]

    def where(ch):
        return ch // SUB, pl.ds(lax.rem(ch, SUB) * T, T)

    def owner(k, e1, e2, e3, c):
        b1, b2, b3 = AXES[k]
        return e1 * b1 + e2 * b2 + e3 * b3 + c

    def send_raw(ch, halves=(0, 1)):
        l, rows = where(ch)
        for half in halves:
            for k in range(3):
                side = bit(AXES[k][0]) if half else 1 - bit(AXES[k][0])
                for q in range(4):
                    j = owner(k, side, q // 2, q % 2, 1 - core)
                    sem = near.at[lax.rem(ch, NEAR)] if half else far.at[lax.rem(ch, RING)]
                    remote(g[k].at[l, j, rows], D.at[k, ch, 4 * side + q], snd.at[0], sem, mate).start()

    def send_first():
        for piece, rows in enumerate(PIECES):
            for k in range(3):
                side = 1 - bit(AXES[k][0])
                sem = early.at[piece, k]
                for q in range(4):
                    j = owner(k, side, q // 2, q % 2, 1 - core)
                    remote(g[k].at[0, j, rows], D.at[k, 0, 4 * side + q, rows], snd.at[0], sem, mate).start()

    def stage1_first():
        loaded(O1.at[0], ld.at[0, 0])
        for piece, rows in enumerate(PIECES):
            for k in range(3):
                b1 = AXES[k][0]
                base = 4 * (1 - bit(b1))
                part = D.at[k, 0, pl.ds(base, 4), rows]
                arrived(part, early.at[piece, k])
                for q in range(4):
                    add_into(D.at[k, 0, base + q, rows], O1.at[0, k, q, rows], D.at[k, 0, base + q, rows])
                remote(part, R1.at[0, k, :, rows], snd.at[0], came(ST1, 0), flip(me, b1)).start()

    def load_own(which, ch):
        l, rows = where(ch)
        slot = lax.rem(ch, 2)
        for k in range(3):
            b1, b2, b3 = AXES[k]
            m1, m2, m3 = bit(b1), bit(b2), bit(b3)
            if which == 0:
                for q in range(4):
                    j = owner(k, 1 - m1, q // 2, q % 2, core)
                    pltpu.make_async_copy(g[k].at[l, j, rows], O1.at[slot, k, q], ld.at[0, slot]).start()
            elif which == 1:
                for q in range(2):
                    j = owner(k, m1, 1 - m2, q, core)
                    pltpu.make_async_copy(g[k].at[l, j, rows], O2.at[slot, k, q], ld.at[1, slot]).start()
            elif which == 2:
                j = owner(k, m1, m2, 1 - m3, core)
                pltpu.make_async_copy(g[k].at[l, j, rows], O3.at[slot, k], ld.at[2, slot]).start()
            else:
                pltpu.make_async_copy(g[k].at[l, me, rows], O4.at[slot, k], ld.at[3, slot]).start()
                pltpu.make_async_copy(w[k].at[l, me, rows], W.at[slot, k], ld.at[4, slot]).start()

    def stage1(ch):
        slot = lax.rem(ch, 2)
        arrived(R1.at[ch], far.at[lax.rem(ch, RING)])
        loaded(O1.at[slot], ld.at[0, slot])
        for k in range(3):
            b1, _, _ = AXES[k]
            base = 4 * (1 - bit(b1))

            def one(q, _):
                add_into(D.at[k, ch, base + q], O1.at[slot, k, q], D.at[k, ch, base + q])
                return 0

            lax.fori_loop(0, 4, one, 0)
            remote(D.at[k, ch, pl.ds(base, 4)], R1.at[ch, k], snd.at[0], came(ST1, ch), flip(me, b1)).start()

    def stage2(ch):
        slot = lax.rem(ch, 2)
        arrived(R1.at[ch], near.at[lax.rem(ch, NEAR)])
        arrived(R1.at[ch], came(ST1, ch))
        loaded(O2.at[slot], ld.at[1, slot])
        for k in range(3):
            b1, b2, _ = AXES[k]
            half = 2 * (1 - bit(b2))
            base = 4 * bit(b1) + half

            def one(q, _):
                add_into(D.at[k, ch, base + q], O2.at[slot, k, q], D.at[k, ch, base + q], R1.at[ch, k, half + q])
                return 0

            lax.fori_loop(0, 2, one, 0)
            remote(D.at[k, ch, pl.ds(base, 2)], R2.at[ch, k], snd.at[0], came(ST2, ch), flip(me, b2)).start()

    def stage3(ch):
        slot = lax.rem(ch, 2)
        arrived(R2.at[ch], came(ST2, ch))
        loaded(O3.at[slot], ld.at[2, slot])
        for k in range(3):
            b1, b2, b3 = AXES[k]
            m1, m2, n3 = bit(b1), bit(b2), 1 - bit(b3)
            mine = D.at[k, ch, 4 * m1 + 2 * m2 + n3]
            add_into(mine, O3.at[slot, k], mine, R1.at[ch, k, 2 * m2 + n3], R2.at[ch, k, n3])
            remote(mine, R3.at[ch, k], snd.at[0], came(ST3, ch), flip(me, b3)).start()

    def give(k, ch, stage, blocks, to):
        l, rows = where(ch)
        recv = a0r.at[lax.min(ch // TAIL, 1)] if stage == AG0 else came(stage, ch)
        for j in blocks:
            part = wo[k].at[l, j, rows]
            remote(part, part, snd.at[1], recv, to).start()

    def update(ch):
        l, rows = where(ch)
        slot = lax.rem(ch, 2)

        @pl.when(ch == 0)
        def _():
            loaded(moments, mv.at[0])

        arrived(R3.at[ch], came(ST3, ch))
        loaded(O4.at[slot], ld.at[3, slot])
        loaded(W.at[slot], ld.at[4, slot])
        for k in range(3):
            b1, b2, b3 = AXES[k]
            m1, m2, m3 = bit(b1), bit(b2), bit(b3)
            total = O4[slot, k].astype(F32)
            for one in (D.at[k, ch, 4 * m1 + 2 * m2 + m3], R1.at[ch, k, 2 * m2 + m3], R2.at[ch, k, m3], R3.at[ch, k]):
                total = total + one[...].astype(F32)
            grad = total.astype(BF16).astype(F32)
            new_m = 0.9 * mo[k][l, rows] + 0.1 * grad
            new_v = 0.95 * vo[k][l, rows] + 0.05 * grad * grad
            old = W[slot, k].astype(F32)
            mo[k][l, rows] = new_m
            vo[k][l, rows] = new_v
            wo[k][l, me, rows] = (old - 0.02 * (new_m * lax.rsqrt(new_v + 1e-8) + 0.1 * old)).astype(BF16)
            give(k, ch, AG3, (me,), flip(me, b3))
            give(k, ch, AG0, (me,), mate)

    def double3(ch):
        arrived(R3.at[ch], came(AG3, ch))
        for k in range(3):
            _, b2, b3 = AXES[k]
            got = flip(me, b3)
            give(k, ch, AG2, (me, got), flip(me, b2))
            give(k, ch, AG0, (got,), mate)

    def double2(ch):
        arrived(R2.at[ch], came(AG2, ch))
        for k in range(3):
            b1, b2, b3 = AXES[k]
            held = (me, flip(me, b3))
            got = tuple(flip(j, b2) for j in held)
            give(k, ch, AG0, got, mate)

            @pl.when(ch >= TAIL)
            def _():
                give(k, ch, AG1, held + got, flip(me, b1))


    def double1(ch):
        l, rows = where(ch)
        arrived(R1.at[ch], came(AG1, ch))
        for k in range(3):
            b1, b2, b3 = AXES[k]
            held = (me, flip(me, b3))
            got = tuple(flip(j, b1) for j in held + tuple(flip(j, b2) for j in held))

            @pl.when(ch < CHUNKS - 1)
            def _():
                give(k, ch, AG0, got, mate)

            @pl.when(ch == CHUNKS - 1)
            def _():
                for q in range(4):
                    mate_part[k, q] = wo[k][l, owner(k, 1 - bit(b1), q // 2, q % 2, core), rows]

    def take_late():
        late = pl.ds(0, TAIL * T)
        arrived(R1.at[pl.ds(0, TAIL)], a0r.at[0])
        for k in range(3):

            @pl.when(core == k - 1 if k else core >= 0)
            def _():
                def one(q, _):
                    if k:
                        split[q] = wo[k][0, owner(k, bit(AXES[k][0]), q // 4, lax.rem(q // 2, 2), lax.rem(q, 2)), late]
                    else:
                        both[q] = wo[k][0, owner(k, bit(AXES[k][0]), q // 2, lax.rem(q, 2), core), late]
                    return 0

                lax.fori_loop(0, 8 if k else 4, one, 0)

    load_own(0, 0)
    for k in range(3):
        pltpu.make_async_copy(m[k], mo[k], mv.at[0]).start()
        pltpu.make_async_copy(v[k], vo[k], mv.at[0]).start()

    barrier = pltpu.get_barrier_semaphore()
    for b in (1, 2, 4, 8):
        pl.semaphore_signal(barrier, inc=1, device_id={"dp": flip(me, b)}, device_id_type=MESH)
    pl.semaphore_wait(barrier, 4)

    send_first()
    send_raw(0, (1,))
    send_raw(1)
    stage1_first()
    send_raw(2)

    def step(s, _):
        def at(lag, do, *args, start=0):
            ch = s - lag

            @pl.when((ch >= start) & (ch < CHUNKS))
            def _():
                do(*args, ch)

        at(0, stage1, start=1)
        at(-LEAD, send_raw, start=LEAD + 1)
        at(-1, load_own, 0)
        at(LAG - 1, load_own, 1)
        at(LAG, load_own, 2)
        at(LAG + 1, load_own, 3)
        at(LAG, stage2)
        at(LAG + 1, stage3)
        at(LAG + 2, update)
        at(LAG + 3, double3)
        at(LAG + 4, double2)
        at(LAG + 5, double1, start=TAIL)
        pl.when(s == CHUNKS)(take_late)
        return 0

    lax.fori_loop(0, CHUNKS + LAG + 5, step, 0)

    arrived(new_w.at[:, :, pl.ds(0, 7), pl.ds(0, 62)], a0r.at[1])
    for i, sent in enumerate((new_w.at[:, :, pl.ds(0, 15)], new_w.at[:, :, pl.ds(0, 14), pl.ds(0, 66)])):
        remote(sent, sent, snd.at[i], a0r.at[0], mate).wait_send()


def run_copies(groups, sem):
    for i, (pairs, _) in enumerate(groups):
        for one, other in pairs:
            pltpu.make_async_copy(one, other, sem.at[i]).start()
    for i, (_, total) in enumerate(groups):
        pltpu.make_async_copy(total, total, sem.at[i]).wait()


def late_blocks(k, far):
    b1, b2, b3 = AXES[k]
    side = lax.rem(lax.axis_index("dp") // b1, 2)
    side = 1 - side if far else side
    return [side * b1 + q // 4 * b2 + q // 2 % 2 * b3 + q % 2 for q in range(8)]


def write_early(moments, new_w, *refs):
    *targets, sem = refs
    late, rest = pl.ds(0, TAIL * T), pl.ds(TAIL * T, TILES - TAIL * T)
    pairs = []
    for k in range(3):
        pairs += [(new_w.at[k, 1], targets[k].at[1]), (new_w.at[k, 0, :, rest], targets[k].at[0, :, rest])]
        pairs += [(new_w.at[k, 0, j, late], targets[k].at[0, j, late]) for j in late_blocks(k, False)]
    small = [(moments.at[i, k], targets[3 + 3 * i + k]) for i in range(2) for k in range(3)]
    run_copies([(pairs, new_w.at[:, :, :, pl.ds(0, TILES - TAIL * T // 4)]), (small, moments)], sem)


def put_late(split, both, targets, core, sem, more=()):
    late = pl.ds(0, TAIL * T)
    far = late_blocks(0, True)
    shared = ([(both.at[q], targets[0].at[0, far[2 * q] + core, late]) for q in range(4)], both)
    for k in (1, 2):

        @pl.when(core == k - 1)
        def _():
            run_copies([*more, shared, ([(split.at[q], targets[k].at[0, j, late]) for q, j in enumerate(late_blocks(k, True))], split)], sem)


def write_next(*refs):
    split, both, last, targets, sem = refs[0], refs[1], refs[2], refs[6:9], refs[9]
    core = lax.rem(lax.axis_index("dp"), 2)
    end, ends = pl.ds(TILES - T, T), []
    for k in range(3):
        far = late_blocks(k, True)
        ends += [(last.at[k, q], targets[k].at[1, far[2 * q] + 1 - core, end]) for q in range(4)]
    put_late(split, both, targets, core, sem, [(ends, last)])


def write_last(*refs):
    split, both, targets, sem = refs[0], refs[1], refs[5:8], refs[8]
    put_late(split, both, targets, 1 - lax.rem(lax.axis_index("dp"), 2), sem)


def tiled(a, parts):
    rows, columns = a.shape[1] // parts // 8, a.shape[2] // 128
    a = a.reshape(LAYERS, parts, rows, 8, columns, 128).transpose(0, 1, 2, 4, 3, 5)
    return a.reshape(LAYERS, parts, TILES, 16, 128)


def untiled(a, shape):
    rows, columns = shape[1] // a.shape[1] // 8, shape[2] // 128
    a = a.reshape(LAYERS, a.shape[1], rows, columns, 8, 128).transpose(0, 1, 2, 4, 3, 5)
    return a.reshape(shape)


def solution(mesh):
    def step(*arrays):
        terms, weights, m, v = (arrays[i : i + 3] for i in (0, 3, 6, 9))
        whole, part = (LAYERS, N, TILES, 16, 128), (LAYERS, TILES, 16, 128)
        block = (T, 16, 128)
        dma = pltpu.SemaphoreType.DMA
        new = pl.pallas_call(
            kernel,
            out_shape=[VM((2, 3, *part), F32), VM((3, *whole), BF16)] + [VM((8, TAIL * T, 16, 128), BF16), VM((4, TAIL * T, 16, 128), BF16), VM((3, 4, *block), BF16)],
            in_specs=[pl.BlockSpec(memory_space=pltpu.HBM)] * 12,
            out_specs=[pl.BlockSpec(memory_space=pltpu.VMEM)] * 5,
            scratch_shapes=[
                pltpu.VMEM((3, CHUNKS, 8, *block), BF16),
                pltpu.VMEM((CHUNKS, 3, 4, *block), BF16),
                pltpu.VMEM((CHUNKS, 3, 2, *block), BF16),
                pltpu.VMEM((CHUNKS, 3, *block), BF16),
                pltpu.VMEM((2, 3, 4, *block), BF16),
                pltpu.VMEM((2, 3, 2, *block), BF16),
                pltpu.VMEM((2, 3, *block), BF16),
                pltpu.VMEM((2, 3, *block), BF16),
                pltpu.VMEM((2, 3, *block), BF16),
                dma((RING,)),
                dma((NEAR,)),
                dma((2, 3)),
                dma((RING1 + 5 * RING,)),
                dma((2,)),
                dma((2,)),
                dma((5, 2)),
                dma((1,)),
            ],
            compiler_params=pltpu.CompilerParams(collective_id=0, has_side_effects=True, vmem_limit_bytes=28 * 2**20),
            name="sum_step_gather",
        )(
            *(tiled(t[0], N) for t in terms),
            *(tiled(one, N) for one in weights),
            *(tiled(one, 1)[:, 0] for one in (*m, *v)),
        )
        moments, new_w, split, both, last = new
        hbm, any_space, vmem = (pl.BlockSpec(memory_space=one) for one in (pltpu.HBM, pl.ANY, pltpu.VMEM))
        out_w, out_m = [jax.ShapeDtypeStruct(whole, BF16)] * 3, [jax.ShapeDtypeStruct(part, F32)] * 6

        def plain(body, out_shape, in_specs, semaphores, aliases, flops):
            return pl.pallas_call(
                body,
                out_shape=out_shape,
                in_specs=in_specs,
                out_specs=[hbm] * len(out_shape),
                scratch_shapes=[dma((semaphores,))],
                input_output_aliases=aliases,
                compiler_params=pltpu.CompilerParams(vmem_limit_bytes=2**20),
                cost_estimate=pl.CostEstimate(flops=flops, bytes_accessed=flops // 100, transcendentals=0),
            )

        split = lax.ppermute(split, "dp", [(i, i ^ (AXES[2][0] if i % 2 else AXES[1][0])) for i in range(N)])
        both = lax.ppermute(both, "dp", [(i, i ^ AXES[0][0]) for i in range(N)])
        last = lax.ppermute(last, "dp", [(i, i ^ 1) for i in range(N)])
        *new_w, m0, m1, m2, v0, v1, v2 = plain(write_early, out_w + out_m, [vmem] * 2, 2, {}, 2 * 10**9)(moments, new_w)
        *new_w, split, both = lax.optimization_barrier((*new_w, split, both))
        mates = [lax.ppermute(one, "dp", [(i, i ^ 1) for i in range(N)]) for one in (split, both)]
        new_w = plain(write_next, out_w, [any_space] * 3 + [hbm] * 3, 3, {3: 0, 4: 1, 5: 2}, 10**9)(split, both, last, *new_w)
        new_w = plain(write_last, out_w, [any_space] * 2 + [hbm] * 3, 2, {2: 0, 3: 1, 4: 2}, 10**9)(*mates, *new_w)
        new = (*new_w, m0, m1, m2, v0, v1, v2)
        return (
            *(untiled(one, w.shape) for one, w in zip(new[:3], weights, strict=True)),
            *(untiled(one[:, None], old.shape) for one, old in zip(new[3:], (*m, *v), strict=True)),
        )

    all_of, cut = P(None, None, None), P(None, "dp", None)
    return jax.shard_map(
        step,
        mesh=mesh,
        in_specs=(P(("rep", "dp"), None, None, None),) * 3 + (all_of,) * 3 + (cut,) * 6,
        out_specs=(P("rep", None, None),) * 3 + (P("rep", "dp", None),) * 6,
        check_vma=False,
    )
```

```python
import jax
import jax.numpy as jnp
from jax import lax
from jax.experimental import pallas as pl
from jax.experimental.pallas import tpu as pltpu
from jax.sharding import PartitionSpec as P


MESH = pl.DeviceIdType.MESH
F32, BF16 = jnp.float32, jnp.bfloat16
N = 16
LAYERS = 2
TILES = 70
AXES = ((4, 2, 8), (2, 8, 4), (8, 4, 2))
SUB = 10
T = TILES // SUB
CHUNKS = LAYERS * SUB
TAIL = 4
PIECES = (pl.ds(0, 2), pl.ds(2, T - 2))
LEAD = 2
LAG = 2
RING, RING1, NEAR = 4, 6, 7
VM = pltpu.VMEM
ST1, ST2, ST3, AG3, AG2, AG1, _, AG0 = range(8)


def add_into(dst, *srcs):
    total = srcs[0][...].astype(F32)
    for one in srcs[1:]:
        total = total + one[...].astype(F32)
    dst[...] = total.astype(BF16)


def kernel(*refs):
    g, w, m, v = (refs[i : i + 3] for i in range(0, 12, 3))
    moments, new_w = refs[12:14]
    split, both, mate_part = refs[14:17]
    wo = [new_w.at[k] for k in range(3)]
    mo, vo = ([moments.at[i, k] for k in range(3)] for i in range(2))
    D, R1, R2, R3, O1, O2, O3, O4, W, far, near, early, rr, a0r, snd, ld, mv = refs[17:]
    me = lax.axis_index("dp")

    def bit(b):
        return lax.rem(me // b, 2)

    def flip(i, b):
        return i + b - 2 * b * bit(b)

    core = bit(1)
    mate = flip(me, 1)

    def remote(src, dst, send, recv, to):
        return pltpu.make_async_remote_copy(src, dst, send, recv, device_id={"dp": to}, device_id_type=MESH)

    def arrived(ref, sem):
        remote(ref, ref, snd.at[0], sem, mate).wait_recv()

    def loaded(ref, sem):
        pltpu.make_async_copy(ref, ref, sem).wait()

    def came(stage, ch):
        return rr.at[lax.rem(ch, RING1) if stage == ST1 else RING1 + RING * (stage - 1) + lax.rem(ch, RING)]

    def where(ch):
        return ch // SUB, pl.ds(lax.rem(ch, SUB) * T, T)

    def owner(k, e1, e2, e3, c):
        b1, b2, b3 = AXES[k]
        return e1 * b1 + e2 * b2 + e3 * b3 + c

    def send_raw(ch, halves=(0, 1)):
        l, rows = where(ch)
        for half in halves:
            for k in range(3):
                side = bit(AXES[k][0]) if half else 1 - bit(AXES[k][0])
                for q in range(4):
                    j = owner(k, side, q // 2, q % 2, 1 - core)
                    sem = near.at[lax.rem(ch, NEAR)] if half else far.at[lax.rem(ch, RING)]
                    remote(g[k].at[l, j, rows], D.at[k, ch, 4 * side + q], snd.at[0], sem, mate).start()

    def send_first():
        for piece, rows in enumerate(PIECES):
            for k in range(3):
                side = 1 - bit(AXES[k][0])
                sem = early.at[piece, k]
                for q in range(4):
                    j = owner(k, side, q // 2, q % 2, 1 - core)
                    remote(g[k].at[0, j, rows], D.at[k, 0, 4 * side + q, rows], snd.at[0], sem, mate).start()

    def stage1_first():
        loaded(O1.at[0], ld.at[0, 0])
        for piece, rows in enumerate(PIECES):
            for k in range(3):
                b1 = AXES[k][0]
                base = 4 * (1 - bit(b1))
                part = D.at[k, 0, pl.ds(base, 4), rows]
                arrived(part, early.at[piece, k])
                for q in range(4):
                    add_into(D.at[k, 0, base + q, rows], O1.at[0, k, q, rows], D.at[k, 0, base + q, rows])
                remote(part, R1.at[0, k, :, rows], snd.at[0], came(ST1, 0), flip(me, b1)).start()

    def load_own(which, ch):
        l, rows = where(ch)
        slot = lax.rem(ch, 2)
        for k in range(3):
            b1, b2, b3 = AXES[k]
            m1, m2, m3 = bit(b1), bit(b2), bit(b3)
            if which == 0:
                for q in range(4):
                    j = owner(k, 1 - m1, q // 2, q % 2, core)
                    pltpu.make_async_copy(g[k].at[l, j, rows], O1.at[slot, k, q], ld.at[0, slot]).start()
            elif which == 1:
                for q in range(2):
                    j = owner(k, m1, 1 - m2, q, core)
                    pltpu.make_async_copy(g[k].at[l, j, rows], O2.at[slot, k, q], ld.at[1, slot]).start()
            elif which == 2:
                j = owner(k, m1, m2, 1 - m3, core)
                pltpu.make_async_copy(g[k].at[l, j, rows], O3.at[slot, k], ld.at[2, slot]).start()
            else:
                pltpu.make_async_copy(g[k].at[l, me, rows], O4.at[slot, k], ld.at[3, slot]).start()
                pltpu.make_async_copy(w[k].at[l, me, rows], W.at[slot, k], ld.at[3, slot]).start()

    def stage1(ch):
        slot = lax.rem(ch, 2)
        arrived(R1.at[ch], far.at[lax.rem(ch, RING)])
        loaded(O1.at[slot], ld.at[0, slot])
        for k in range(3):
            b1, _, _ = AXES[k]
            base = 4 * (1 - bit(b1))

            def one(q, _):
                add_into(D.at[k, ch, base + q], O1.at[slot, k, q], D.at[k, ch, base + q])
                return 0

            lax.fori_loop(0, 4, one, 0)
            remote(D.at[k, ch, pl.ds(base, 4)], R1.at[ch, k], snd.at[0], came(ST1, ch), flip(me, b1)).start()

    def stage2(ch):
        slot = lax.rem(ch, 2)
        arrived(R1.at[ch], near.at[lax.rem(ch, NEAR)])
        arrived(R1.at[ch], came(ST1, ch))
        loaded(O2.at[slot], ld.at[1, slot])
        for k in range(3):
            b1, b2, _ = AXES[k]
            half = 2 * (1 - bit(b2))
            base = 4 * bit(b1) + half

            def one(q, _):
                add_into(D.at[k, ch, base + q], O2.at[slot, k, q], D.at[k, ch, base + q], R1.at[ch, k, half + q])
                return 0

            lax.fori_loop(0, 2, one, 0)
            remote(D.at[k, ch, pl.ds(base, 2)], R2.at[ch, k], snd.at[0], came(ST2, ch), flip(me, b2)).start()

    def stage3(ch):
        slot = lax.rem(ch, 2)
        arrived(R2.at[ch], came(ST2, ch))
        loaded(O3.at[slot], ld.at[2, slot])
        for k in range(3):
            b1, b2, b3 = AXES[k]
            m1, m2, n3 = bit(b1), bit(b2), 1 - bit(b3)
            mine = D.at[k, ch, 4 * m1 + 2 * m2 + n3]
            add_into(mine, O3.at[slot, k], mine, R1.at[ch, k, 2 * m2 + n3], R2.at[ch, k, n3])
            remote(mine, R3.at[ch, k], snd.at[0], came(ST3, ch), flip(me, b3)).start()

    def give(k, ch, stage, blocks, to):
        l, rows = where(ch)
        recv = a0r.at[lax.min(ch // TAIL, 1)] if stage == AG0 else came(stage, ch)
        for j in blocks:
            part = wo[k].at[l, j, rows]
            remote(part, part, snd.at[1], recv, to).start()

    def update(ch):
        l, rows = where(ch)
        slot = lax.rem(ch, 2)

        @pl.when(ch == 0)
        def _():
            loaded(moments, mv.at[0])

        arrived(R3.at[ch], came(ST3, ch))
        loaded(O1.at[slot, :, pl.ds(0, 2)], ld.at[3, slot])
        for k in range(3):
            b1, b2, b3 = AXES[k]
            m1, m2, m3 = bit(b1), bit(b2), bit(b3)
            total = O4[slot, k].astype(F32)
            for one in (D.at[k, ch, 4 * m1 + 2 * m2 + m3], R1.at[ch, k, 2 * m2 + m3], R2.at[ch, k, m3], R3.at[ch, k]):
                total = total + one[...].astype(F32)
            grad = total.astype(BF16).astype(F32)
            new_m = 0.9 * mo[k][l, rows] + 0.1 * grad
            new_v = 0.95 * vo[k][l, rows] + 0.05 * grad * grad
            old = W[slot, k].astype(F32)
            mo[k][l, rows] = new_m
            vo[k][l, rows] = new_v
            wo[k][l, me, rows] = (old - 0.02 * (new_m * lax.rsqrt(new_v + 1e-8) + 0.1 * old)).astype(BF16)
            give(k, ch, AG3, (me,), flip(me, b3))
            give(k, ch, AG0, (me,), mate)

    def double3(ch):
        arrived(R3.at[ch], came(AG3, ch))
        for k in range(3):
            _, b2, b3 = AXES[k]
            got = flip(me, b3)
            give(k, ch, AG2, (me, got), flip(me, b2))
            give(k, ch, AG0, (got,), mate)

    def double2(ch):
        l, rows = where(ch)
        arrived(R2.at[ch], came(AG2, ch))
        for k in range(3):
            b1, b2, b3 = AXES[k]
            held = (me, flip(me, b3))
            got = tuple(flip(j, b2) for j in held)
            give(k, ch, AG0, got, mate)

            @pl.when((ch >= TAIL) & (ch < CHUNKS - 1))
            def _():
                give(k, ch, AG1, held + got, flip(me, b1))

            @pl.when(ch == CHUNKS - 1)
            def _():
                for q in range(4):
                    part = wo[k].at[l, owner(k, bit(b1), q // 2, q % 2, core), rows]
                    remote(part, mate_part.at[k, q], snd.at[1], came(AG1, ch), flip(me, b1)).start()


    def double1(ch):
        l, rows = where(ch)
        arrived(R1.at[ch], came(AG1, ch))
        for k in range(3):
            b1, b2, b3 = AXES[k]
            held = (me, flip(me, b3))
            got = tuple(flip(j, b1) for j in held + tuple(flip(j, b2) for j in held))

            @pl.when(ch < CHUNKS - 1)
            def _():
                give(k, ch, AG0, got, mate)

    def take_late():
        late = pl.ds(0, TAIL * T)
        arrived(R1.at[pl.ds(0, TAIL)], a0r.at[0])
        for k in range(3):

            @pl.when(core == k - 1 if k else core >= 0)
            def _():
                def one(q, _):
                    if k:
                        split[q] = wo[k][0, owner(k, bit(AXES[k][0]), q // 4, lax.rem(q // 2, 2), lax.rem(q, 2)), late]
                    else:
                        both[q] = wo[k][0, owner(k, bit(AXES[k][0]), q // 2, lax.rem(q, 2), core), late]
                    return 0

                lax.fori_loop(0, 8 if k else 4, one, 0)

    load_own(0, 0)
    for k in range(3):
        pltpu.make_async_copy(m[k], mo[k], mv.at[0]).start()
        pltpu.make_async_copy(v[k], vo[k], mv.at[0]).start()

    barrier = pltpu.get_barrier_semaphore()
    for b in (1, 2, 4, 8):
        pl.semaphore_signal(barrier, inc=1, device_id={"dp": flip(me, b)}, device_id_type=MESH)
    pl.semaphore_wait(barrier, 4)

    send_first()
    send_raw(0, (1,))
    send_raw(1)
    stage1_first()
    send_raw(2)

    def step(s, _):
        def at(lag, do, *args, start=0):
            ch = s - lag

            @pl.when((ch >= start) & (ch < CHUNKS))
            def _():
                do(*args, ch)

        at(0, stage1, start=1)
        at(-LEAD, send_raw, start=LEAD + 1)
        at(-1, load_own, 0)
        at(LAG - 1, load_own, 1)
        at(LAG, load_own, 2)
        at(LAG + 1, load_own, 3)
        at(LAG, stage2)
        at(LAG + 1, stage3)
        at(LAG + 2, update)
        at(LAG + 3, double3)
        at(LAG + 4, double2)
        at(LAG + 5, double1, start=TAIL)
        pl.when(s == CHUNKS)(take_late)
        return 0

    lax.fori_loop(0, CHUNKS + LAG + 5, step, 0)

    arrived(new_w.at[:, :, pl.ds(0, 7), pl.ds(0, 62)], a0r.at[1])
    for i, sent in enumerate((new_w.at[:, :, pl.ds(0, 15)], new_w.at[:, :, pl.ds(0, 14), pl.ds(0, 66)])):
        remote(sent, sent, snd.at[i], a0r.at[0], mate).wait_send()


def run_copies(groups, sem):
    for i, (pairs, _) in enumerate(groups):
        for one, other in pairs:
            pltpu.make_async_copy(one, other, sem.at[i]).start()
    for i, (_, total) in enumerate(groups):
        pltpu.make_async_copy(total, total, sem.at[i]).wait()


def late_blocks(k, far):
    b1, b2, b3 = AXES[k]
    side = lax.rem(lax.axis_index("dp") // b1, 2)
    side = 1 - side if far else side
    return [side * b1 + q // 4 * b2 + q // 2 % 2 * b3 + q % 2 for q in range(8)]


def write_early(moments, new_w, *refs):
    *targets, sem = refs
    late, rest = pl.ds(0, TAIL * T), pl.ds(TAIL * T, TILES - TAIL * T)
    pairs = []
    for k in range(3):
        pairs += [(new_w.at[k, 1], targets[k].at[1]), (new_w.at[k, 0, :, rest], targets[k].at[0, :, rest])]
        pairs += [(new_w.at[k, 0, j, late], targets[k].at[0, j, late]) for j in late_blocks(k, False)]
    small = [(moments.at[i, k], targets[3 + 3 * i + k]) for i in range(2) for k in range(3)]
    run_copies([(pairs, new_w.at[:, :, :, pl.ds(0, TILES - TAIL * T // 4)]), (small, moments)], sem)


def put_late(split, both, targets, core, sem, more=()):
    late = pl.ds(0, TAIL * T)
    far = late_blocks(0, True)
    shared = ([(both.at[q], targets[0].at[0, far[2 * q] + core, late]) for q in range(4)], both)
    for k in (1, 2):

        @pl.when(core == k - 1)
        def _():
            run_copies([*more, shared, ([(split.at[q], targets[k].at[0, j, late]) for q, j in enumerate(late_blocks(k, True))], split)], sem)


def write_next(*refs):
    split, both, last, own, targets, sem = *refs[0:4], refs[7:10], refs[10]
    core = lax.rem(lax.axis_index("dp"), 2)
    end, ends, own_ends = pl.ds(TILES - T, T), [], []
    for k in range(3):
        far = late_blocks(k, True)
        ends += [(last.at[k, q], targets[k].at[1, far[2 * q] + 1 - core, end]) for q in range(4)]
        own_ends += [(own.at[k, q], targets[k].at[1, far[2 * q] + core, end]) for q in range(4)]
    put_late(split, both, targets, core, sem, [(ends, last), (own_ends, own)])


def write_last(*refs):
    split, both, targets, sem = refs[0], refs[1], refs[5:8], refs[8]
    put_late(split, both, targets, 1 - lax.rem(lax.axis_index("dp"), 2), sem)


def tiled(a, parts):
    rows, columns = a.shape[1] // parts // 8, a.shape[2] // 128
    a = a.reshape(LAYERS, parts, rows, 8, columns, 128).transpose(0, 1, 2, 4, 3, 5)
    return a.reshape(LAYERS, parts, TILES, 16, 128)


def untiled(a, shape):
    rows, columns = shape[1] // a.shape[1] // 8, shape[2] // 128
    a = a.reshape(LAYERS, a.shape[1], rows, columns, 8, 128).transpose(0, 1, 2, 4, 3, 5)
    return a.reshape(shape)


def solution(mesh):
    def step(*arrays):
        terms, weights, m, v = (arrays[i : i + 3] for i in (0, 3, 6, 9))
        whole, part = (LAYERS, N, TILES, 16, 128), (LAYERS, TILES, 16, 128)
        block = (T, 16, 128)
        dma = pltpu.SemaphoreType.DMA
        new = pl.pallas_call(
            kernel,
            out_shape=[VM((2, 3, *part), F32), VM((3, *whole), BF16)] + [VM((8, TAIL * T, 16, 128), BF16), VM((4, TAIL * T, 16, 128), BF16), VM((3, 4, *block), BF16)],
            in_specs=[pl.BlockSpec(memory_space=pltpu.HBM)] * 12,
            out_specs=[pl.BlockSpec(memory_space=pltpu.VMEM)] * 5,
            scratch_shapes=[
                pltpu.VMEM((3, CHUNKS, 8, *block), BF16),
                pltpu.VMEM((CHUNKS, 3, 4, *block), BF16),
                pltpu.VMEM((CHUNKS, 3, 2, *block), BF16),
                pltpu.VMEM((CHUNKS, 3, *block), BF16),
                pltpu.VMEM((2, 3, 4, *block), BF16),
                pltpu.VMEM((2, 3, 2, *block), BF16),
                pltpu.VMEM((2, 3, *block), BF16),
                pltpu.VMEM((2, 3, *block), BF16),
                pltpu.VMEM((2, 3, *block), BF16),
                dma((RING,)),
                dma((NEAR,)),
                dma((2, 3)),
                dma((RING1 + 5 * RING,)),
                dma((2,)),
                dma((2,)),
                dma((4, 2)),
                dma((1,)),
            ],
            compiler_params=pltpu.CompilerParams(collective_id=0, has_side_effects=True, vmem_limit_bytes=28 * 2**20),
            name="sum_step_gather",
        )(
            *(tiled(t[0], N) for t in terms),
            *(tiled(one, N) for one in weights),
            *(tiled(one, 1)[:, 0] for one in (*m, *v)),
        )
        moments, new_w, split, both, last = new
        hbm, any_space, vmem = (pl.BlockSpec(memory_space=one) for one in (pltpu.HBM, pl.ANY, pltpu.VMEM))
        out_w, out_m = [jax.ShapeDtypeStruct(whole, BF16)] * 3, [jax.ShapeDtypeStruct(part, F32)] * 6

        def plain(body, out_shape, in_specs, semaphores, aliases, flops):
            return pl.pallas_call(
                body,
                out_shape=out_shape,
                in_specs=in_specs,
                out_specs=[hbm] * len(out_shape),
                scratch_shapes=[dma((semaphores,))],
                input_output_aliases=aliases,
                compiler_params=pltpu.CompilerParams(vmem_limit_bytes=2**20),
                cost_estimate=pl.CostEstimate(flops=flops, bytes_accessed=flops // 100, transcendentals=0),
            )

        split = lax.ppermute(split, "dp", [(i, i ^ (AXES[2][0] if i % 2 else AXES[1][0])) for i in range(N)])
        both = lax.ppermute(both, "dp", [(i, i ^ AXES[0][0]) for i in range(N)])
        own_last = last
        last = lax.ppermute(last, "dp", [(i, i ^ 1) for i in range(N)])
        *new_w, m0, m1, m2, v0, v1, v2 = plain(write_early, out_w + out_m, [vmem] * 2, 2, {}, 2 * 10**9)(moments, new_w)
        *new_w, split, both = lax.optimization_barrier((*new_w, split, both))
        mates = [lax.ppermute(one, "dp", [(i, i ^ 1) for i in range(N)]) for one in (split, both)]
        new_w = plain(write_next, out_w, [any_space] * 4 + [hbm] * 3, 4, {4: 0, 5: 1, 6: 2}, 10**9)(split, both, last, own_last, *new_w)
        new_w = plain(write_last, out_w, [any_space] * 2 + [hbm] * 3, 2, {2: 0, 3: 1, 4: 2}, 10**9)(*mates, *new_w)
        new = (*new_w, m0, m1, m2, v0, v1, v2)
        return (
            *(untiled(one, w.shape) for one, w in zip(new[:3], weights, strict=True)),
            *(untiled(one[:, None], old.shape) for one, old in zip(new[3:], (*m, *v), strict=True)),
        )

    all_of, cut = P(None, None, None), P(None, "dp", None)
    return jax.shard_map(
        step,
        mesh=mesh,
        in_specs=(P(("rep", "dp"), None, None, None),) * 3 + (all_of,) * 3 + (cut,) * 6,
        out_specs=(P("rep", None, None),) * 3 + (P("rep", "dp", None),) * 6,
        check_vma=False,
    )
```
